32 devices in a mesh: dp: 2 (over x), tp: 16 (over y, z, core).
Axes of the slice: x: 2, y: 2, z: 4, core: 2. Of those that a mesh axis runs over, the one named last changes fastest.
Arguments:
- x: bfloat16 [4096, 5120], P('dp'), parts along dimension 0
- dy: bfloat16 [4096, 5120], P('dp'), parts along dimension 0
- gate: bfloat16 [4096, 14336], P('dp', 'tp'), parts along dimension 0
- up: bfloat16 [4096, 14336], P('dp', 'tp'), parts along dimension 0
- w_gate: bfloat16 [5120, 14336], P(None, 'tp')
- w_up: bfloat16 [5120, 14336], P(None, 'tp')
- w_down: bfloat16 [14336, 5120], P('tp')
Outputs:
- output 1: bfloat16 [4096, 5120], P('dp'), parts along dimension 0
- output 2: bfloat16 [10240, 14336], P('dp', 'tp'), parts along dimension 0
- output 3: bfloat16 [10240, 14336], P('dp', 'tp'), parts along dimension 0
- output 4: bfloat16 [28672, 5120], P(('dp', 'tp')), parts along dimension 0
There are 2 independent parts. The reference program is written for one: setup_inputs(seed, part) draws one part's arguments, and reference() takes and returns one part's arrays. A program takes and returns all parts, laid end to end along the dimension named above; an argument that names none is the same for every part.
All inputs are finite; a program needn't handle non-finite values.
Results may differ from the reference program's by a relative error of at most 0.012.
Values are sent between devices in bfloat16 or wider.
A program may use at most 2 GiB of HBM per device.

```python
import jax
import jax.numpy as jnp

ROWS = 2048
D = 5120
FF = 14336


def act(gate, up):
    return jax.nn.silu(gate) * up


def setup_inputs(seed: int = 0, part: int = 0) -> dict:
    kx, ky, ka, kb, kg, ku, kd = jax.random.split(jax.random.key(seed), 7)
    kx, ky, ka, kb = (jax.random.fold_in(k, part) for k in (kx, ky, ka, kb))
    drawn = {
        "x": jax.random.normal(kx, (ROWS, D), jnp.float32),
        "dy": jax.random.normal(ky, (ROWS, D), jnp.float32),
        "gate": jax.random.normal(ka, (ROWS, FF), jnp.float32),
        "up": jax.random.normal(kb, (ROWS, FF), jnp.float32),
        "w_gate": jax.random.normal(kg, (D, FF), jnp.float32) * D**-0.5,
        "w_up": jax.random.normal(ku, (D, FF), jnp.float32) * D**-0.5,
        "w_down": jax.random.normal(kd, (FF, D), jnp.float32) * FF**-0.5,
    }
    return {k: v.astype(jnp.bfloat16) for k, v in drawn.items()}


def reference(x, dy, gate, up, w_gate, w_up, w_down):
    hidden, back = jax.vjp(act, gate.astype(jnp.float32), up.astype(jnp.float32))
    d_hidden = jnp.dot(dy, w_down.T, preferred_element_type=jnp.float32)
    d_gate, d_up = (g.astype(jnp.bfloat16) for g in back(d_hidden))
    dx = jnp.dot(d_gate, w_gate.T, preferred_element_type=jnp.float32) + jnp.dot(d_up, w_up.T, preferred_element_type=jnp.float32)
    dw_gate = jnp.dot(x.T, d_gate, preferred_element_type=jnp.float32)
    dw_up = jnp.dot(x.T, d_up, preferred_element_type=jnp.float32)
    dw_down = jnp.dot(hidden.astype(jnp.bfloat16).T, dy, preferred_element_type=jnp.float32)
    return tuple(g.astype(jnp.bfloat16) for g in (dx, dw_gate, dw_up, dw_down))
```

```python
import jax
import jax.numpy as jnp
from jax import lax
from jax.experimental import pallas as pl
from jax.experimental.pallas import tpu as pltpu
from jax.sharding import PartitionSpec as P

MESH = pl.DeviceIdType.MESH
bf, f32 = jnp.bfloat16, jnp.float32
DMA = pltpu.SemaphoreType.DMA
L = 128

T_ROWS, D_MODEL, FF = 2048, 5120, 896
HC = D_MODEL // 2
A, A2, BO, BT, MC = 6 * L, 3 * L, 12 * L, 2 * L, 14 * L

R, D = 32, 2
NB = T_ROWS // R
NS, NR, W = 2 * D, 8 * D, 2
STEPS = NB + 8 * D
FILL, DRAIN = 4 * D, NB + 3 * D

G = 256
NG, BPG, PPG = T_ROWS // G, G // R, 6
LEAD = PPG
Q = D_MODEL // 4
F0 = 512
XT, YT = 256, 512
NX, NY = D_MODEL // XT, D_MODEL // YT
P2 = NG * PPG
PIECES2 = NX + NY


def dot(a, b, ca, cb):
    return lax.dot_general(a, b, (((ca,), (cb,)), ((), ())), preferred_element_type=f32)


SCRATCH = dict(
    WD=pltpu.VMEM((FF, D_MODEL), bf),
    WGU=pltpu.VMEM((D_MODEL, 2 * FF), bf),
    DGU=pltpu.VMEM((T_ROWS, 2 * FF), bf),
    HID=pltpu.VMEM((T_ROWS, FF), bf),
    DY=pltpu.VMEM((2, G, D_MODEL), bf),
    GA=pltpu.VMEM((2, G, FF), bf),
    UP=pltpu.VMEM((2, G, FF), bf),
    PST=pltpu.VMEM((2, G, Q), bf),
    OST=pltpu.VMEM((2, G, Q), f32),
    H=pltpu.VMEM((NR, R, HC), f32),
    PT=pltpu.VMEM((4, R, HC), bf),
    F=pltpu.VMEM((NR, R, HC), bf),
    SR=pltpu.VMEM((NS, R, MC), bf),
    SL=pltpu.VMEM((NS, R, MC), bf),
    SY=pltpu.VMEM((NS, R, MC), bf),
    RR=pltpu.VMEM((NS, R, MC), bf),
    RL=pltpu.VMEM((NS, R, MC), bf),
    RY=pltpu.VMEM((NS, R, MC), bf),
    ss=DMA((3, NS)),
    rs=DMA((3, NS)),
    lh=DMA((4,)),
    lp=DMA((4,)),
    os=DMA((4,)),
    ds=DMA((4,)),
    dr=DMA((4,)),
    wd=DMA((1,)),
    wgu=DMA((4, 2)),
    ld=DMA((2, 3)),
    ps=DMA((2,)),
    pr=DMA((NG, 2)),
    ow=DMA((2,)),
    xl=DMA((2,)),
    yl=DMA((2,)),
    xo=DMA((2, 2)),
    yo=DMA((2,)),
)


OPERANDS = ("x", "dy", "gate", "up", "wg", "wu", "wd_h", "dx", "dwg", "dwu", "dwd", "own", "pt")


class Kernel:
    def __init__(s, *refs):
        s.__dict__.update(zip(OPERANDS + tuple(SCRATCH), refs, strict=True))
        i = lax.axis_index("tp")
        s.y, s.z, s.c = i // 8, lax.rem(i // 2, 4), lax.rem(i, 2)
        s.zm = 3 - s.z
        s.yid, s.cid = i + 8 - 16 * s.y, i + 1 - 2 * s.c
        s.rid, s.lid = jnp.minimum(i + 2, 15), jnp.maximum(i - 2, 0)
        s.has_r, s.has_l = s.z < 3, s.z > 0
        m = pl.multiple_of
        s.a0, s.o0 = m(s.y * A, L), m((1 - s.y) * A, L)
        s.a3, s.o3 = m(s.a0 + A2, L), m(s.o0 + A2, L)
        bz = BO + s.z * BT
        s.b_own, s.b_oth = m(bz + s.y * L, L), m(bz + (1 - s.y) * L, L)
        s.half = m(s.c * HC, HC)

    def barrier(s):
        b = pltpu.get_barrier_semaphore()

        def greet(d):
            pl.semaphore_signal(b, inc=1, device_id={"tp": d}, device_id_type=MESH)

        greet(s.yid)
        greet(s.cid)
        pl.when(s.has_r)(lambda: greet(s.rid))
        pl.when(s.has_l)(lambda: greet(s.lid))
        both = s.has_r & s.has_l
        pl.when(both)(lambda: pl.semaphore_wait(b, 4))
        pl.when(jnp.logical_not(both))(lambda: pl.semaphore_wait(b, 3))


    def loads(s, b):
        rows = pl.ds(pl.multiple_of(b * R, R), R)
        k = lax.rem(b, 4)
        return (
            pltpu.make_async_copy(s.own.at[rows], s.H.at[lax.rem(b, NR)], s.lh.at[k]),
            pltpu.make_async_copy(s.pt.at[rows], s.PT.at[k], s.lp.at[k]),
        )

    def start_loads(s, b):
        for c in s.loads(b):
            c.start()

    def message(s, link, t, kind):
        k = lax.rem(t, NS)
        lo, hi = (
            ((5 * L, MC), (0, 9 * L), (0, 7 * L)),
            ((0, MC),) * 3,
            ((0, 9 * L), (5 * L, MC), (7 * L, MC)),
        )[kind][link]
        src, dst = ((s.SR, s.RR), (s.SL, s.RL), (s.SY, s.RY))[link]
        at = (k, slice(None), pl.ds(lo, hi - lo))
        return pltpu.make_async_remote_copy(
            src_ref=src.at[at],
            dst_ref=dst.at[at],
            send_sem=s.ss.at[link, k],
            recv_sem=s.rs.at[link, k],
            device_id={"tp": (s.rid, s.lid, s.yid)[link]},
            device_id_type=MESH,
        )

    def messages(s, t, valid, do, right, left):
        def kind(k):
            do(s.message(2, t, k))
            pl.when(right)(lambda: do(s.message(0, t, k)))
            pl.when(left)(lambda: do(s.message(1, t, k)))

        pl.when(valid & (t < FILL))(lambda: kind(0))
        pl.when(valid & (t >= FILL) & (t < DRAIN))(lambda: kind(1))
        pl.when(valid & (t >= DRAIN) & (t < STEPS - D))(lambda: kind(2))

    def outs(s, b):
        k, q = lax.rem(b, NR), lax.rem(b, 4)
        dst = s.dx.at[pl.ds(pl.multiple_of(b * R, R), R), pl.ds(s.half, HC)]
        return (
            pltpu.make_async_copy(s.F.at[k], dst, s.os.at[q]),
            pltpu.make_async_remote_copy(
                src_ref=s.F.at[k],
                dst_ref=dst,
                send_sem=s.ds.at[q],
                recv_sem=s.dr.at[q],
                device_id={"tp": s.cid},
                device_id_type=MESH,
            ),
        )

    def wait_outs(s, b):
        for c in s.outs(b):
            c.wait()

    def service(s, t):
        s.messages(t - D, t >= D, lambda c: c.wait_recv(), s.has_l, s.has_r)
        s.messages(t - NS, t >= NS, lambda c: c.wait_send(), s.has_r, s.has_l)

        @pl.when(t < NB)
        def _():
            for c in s.loads(t):
                c.wait()

        @pl.when(t + 2 < NB)
        def _():
            g = (t + 2) // BPG
            pl.when(lax.rem(t + 2, BPG) == 0)(lambda: s.wait_partner(g))
            s.start_loads(t + 2)

        pl.when(t >= 8 * D + W)(lambda: s.wait_outs(t - 8 * D - W))

        def h(o):
            return lax.rem(t - o + 4 * NR, NR)

        H, F, z, zm = s.H, s.F, s.z, s.zm
        k, kr = lax.rem(t, NS), lax.rem(t + NS - D, NS)
        RY, RR, RL = s.RY.at[kr], s.RR.at[kr], s.RL.at[kr]
        SY, SR, SL = s.SY.at[k], s.SR.at[k], s.SL.at[k]

        H[h(0)] = H[h(0)] + s.PT[lax.rem(t, 4)].astype(f32)
        own = (h(D), slice(None), pl.ds(s.a0, A))
        H[own] = H[own] + RY[:, 0 : 6 * L].astype(f32)
        rooted = (h(4 * D), slice(None), pl.ds(s.b_own, L))
        F[rooted] = (H[rooted] + RY[:, 6 * L : 7 * L].astype(f32)).astype(bf)
        F[h(5 * D), :, pl.ds(s.b_oth, L)] = RY[:, 7 * L : 8 * L]
        F[h(5 * D + D * z), :, pl.ds(s.o0, A2)] = RY[:, 8 * L : 11 * L]
        F[h(5 * D + D * zm), :, pl.ds(s.o3, A2)] = RY[:, 11 * L : 14 * L]
        to_r = jnp.where(s.has_l, RR[:, 11 * L :].astype(f32), 0.0) + H[h(D + D * z), :, pl.ds(s.a3, A2)]
        to_l = jnp.where(s.has_r, RL[:, : 3 * L].astype(f32), 0.0) + H[h(D + D * zm), :, pl.ds(s.a0, A2)]
        to_r, to_l = to_r.astype(bf), to_l.astype(bf)
        f3 = jnp.where(s.has_r, RL[:, 11 * L :], to_r)
        f0 = jnp.where(s.has_l, RR[:, : 3 * L], to_l)
        F[h(4 * D + D * zm), :, pl.ds(s.a3, A2)] = f3
        F[h(4 * D + D * z), :, pl.ds(s.a0, A2)] = f0
        SR[:, 11 * L :], SR[:, : 3 * L] = to_r, f0
        SL[:, : 3 * L], SL[:, 11 * L :] = to_l, f3
        SY[:, 8 * L : 11 * L], SY[:, 11 * L :] = f0, f3
        hr, hl = h(D * z), h(D * zm)
        for q in range(4):
            b = pl.ds(BO + q * BT, BT)
            m = pl.ds(3 * L + q * BT, BT)
            rr, rl = RR[:, m], RL[:, m]
            sum_r = H[hr, :, b] + jnp.where(s.has_l, rr.astype(f32), 0.0)

            @pl.when(z == q)
            def _():
                H[hr, :, b] = sum_r

            sum_l = H[hl, :, b] + jnp.where(s.has_r, rl.astype(f32), 0.0)

            @pl.when(z == q)
            def _():
                H[hl, :, b] = sum_l

            fq = h(5 * D + D * jnp.abs(z - q))

            @pl.when(z > q)
            def _():
                F[fq, :, b] = rr

            @pl.when(z < q)
            def _():
                F[fq, :, b] = rl

            done = F[fq, :, b]
            SR[:, m] = jnp.where(z >= q, done, sum_r.astype(bf))
            SL[:, m] = jnp.where(z <= q, done, sum_l.astype(bf))
        SY[:, : 6 * L] = H[h(0), :, pl.ds(s.o0, A)].astype(bf)
        SY[:, 6 * L : 7 * L] = H[h(3 * D), :, pl.ds(s.b_oth, L)].astype(bf)
        SY[:, 7 * L : 8 * L] = F[h(4 * D), :, pl.ds(s.b_own, L)]
        s.messages(t, t >= 0, lambda c: c.start(), s.has_r, s.has_l)

        @pl.when(t >= 8 * D)
        def _():
            for c in s.outs(t - 8 * D):
                c.start()

    def finish(s):
        for b in range(NB - W, NB):
            s.wait_outs(b)
        for t in range(STEPS - D - NS + D, STEPS - D):
            s.message(2, t, 2).wait_send()
            pl.when(s.has_r)(lambda t=t: s.message(0, t, 2).wait_send())
            pl.when(s.has_l)(lambda t=t: s.message(1, t, 2).wait_send())


    def weights(s):
        def copy(src, dst, sem):
            return pltpu.make_async_copy(src, dst, sem)

        first = copy(s.wd_h, s.WD, s.wd.at[0])
        quarters = []
        for j in range(4):
            rows = pl.ds(s.quarter(j), Q)
            quarters.append(
                [
                    copy(w.at[rows], s.WGU.at[rows, pl.ds(n * FF, FF)], s.wgu.at[j, n])
                    for n, w in enumerate((s.wg, s.wu))
                ]
            )
        return first, quarters

    def quarter(s, j):
        mine = jnp.where(j < 2, 1 - s.c, s.c)
        return pl.multiple_of(mine * HC + lax.rem(j, 2) * Q, Q)

    def group_loads(s, g):
        k = lax.rem(g, 2)
        rows = pl.ds(pl.multiple_of(g * G, G), G)
        return [
            pltpu.make_async_copy(a.at[rows], v.at[k], s.ld.at[k, n])
            for n, (a, v) in enumerate(((s.dy, s.DY), (s.gate, s.GA), (s.up, s.UP)))
        ]

    def to_partner(s, g, j):
        rows = pl.ds(pl.multiple_of(g * G, G), G)
        return pltpu.make_async_remote_copy(
            src_ref=s.PST.at[j],
            dst_ref=s.pt.at[rows, pl.ds(pl.multiple_of(j * Q, Q), Q)],
            send_sem=s.ps.at[j],
            recv_sem=s.pr.at[g, j],
            device_id={"tp": s.cid},
            device_id_type=MESH,
        )

    def to_own(s, g, j):
        rows = pl.ds(pl.multiple_of(g * G, G), G)
        dst = s.own.at[rows, pl.ds(pl.multiple_of(j * Q, Q), Q)]
        return pltpu.make_async_copy(s.OST.at[j], dst, s.ow.at[j])

    def wait_partner(s, g):
        for j in range(2):
            s.to_partner(g, j).wait_recv()

    def hidden(s, g, lo, hi):
        k = lax.rem(g, 2)
        rows = pl.ds(pl.multiple_of(g * G, G), G)
        d = dot(s.DY[k], s.WD[lo:hi, :], 1, 1)
        a, u = s.GA[k, :, lo:hi].astype(f32), s.UP[k, :, lo:hi].astype(f32)
        sig = jax.nn.sigmoid(a)
        silu = a * sig
        s.DGU[rows, lo:hi] = (d * u * (sig + silu * (1.0 - sig))).astype(bf)
        s.DGU[rows, FF + lo : FF + hi] = (d * silu).astype(bf)
        s.HID[rows, lo:hi] = (silu * u).astype(bf)

    def term(s, g, j):
        rows = pl.ds(pl.multiple_of(g * G, G), G)
        return dot(s.DGU[rows, :], s.WGU[pl.ds(s.quarter(j), Q), :], 1, 1)

    def before1(s, u):
        g = u // PPG

        @pl.when(u > 0)
        def _():
            for j in range(2):
                s.to_partner(g - 1, j).wait_send()
                s.to_own(g - 1, j).wait()

        @pl.when(u == LEAD)
        def _():
            s.wait_partner(0)
            s.start_loads(0)
            s.start_loads(1)

        @pl.when(g + 1 < NG)
        def _():
            for c in s.group_loads(g + 1):
                c.start()

    def piece1(s, u):
        g, r = u // PPG, lax.rem(u, PPG)
        first, quarters = s.weights()

        @pl.when(r == 0)
        def _():
            for c in s.group_loads(g):
                c.wait()
            pl.when(g == 0)(lambda: first.wait())
            s.hidden(g, 0, F0)

        pl.when(r == 1)(lambda: s.hidden(g, F0, FF))
        for j in range(4):

            @pl.when(u == 2 + j)
            def _(j=j):
                for c in quarters[j]:
                    c.wait()

        @pl.when((r == 2) | (r == 3))
        def _():
            j = r - 2
            s.PST[j] = s.term(g, r - 2).astype(bf)
            s.to_partner(g, j).start()

        @pl.when(r >= 4)
        def _():
            j = r - 4
            s.OST[j] = s.term(g, r - 2)
            s.to_own(g, j).start()


    def x_tile(s, q):
        k = lax.rem(q, 2)
        v = s.WGU.at[pl.ds(0, T_ROWS), pl.ds(pl.multiple_of(k * XT, XT), XT)]
        src = s.x.at[:, pl.ds(pl.multiple_of(q * XT, XT), XT)]
        return v, pltpu.make_async_copy(src, v, s.xl.at[k])

    def y_tile(s, q):
        k = lax.rem(q, 2)
        v = s.WGU.at[pl.ds(T_ROWS, T_ROWS), pl.ds(pl.multiple_of(k * YT, YT), YT)]
        src = s.dy.at[:, pl.ds(pl.multiple_of(q * YT, YT), YT)]
        return v, pltpu.make_async_copy(src, v, s.yl.at[k])

    def x_out(s, q):
        k = lax.rem(q, 2)
        v = s.WGU.at[pl.ds(pl.multiple_of(2 * T_ROWS + k * XT, XT), XT), :]
        rows = pl.ds(pl.multiple_of(q * XT, XT), XT)
        return v, [
            pltpu.make_async_copy(v.at[:, pl.ds(n * FF, FF)], o.at[rows], s.xo.at[k, n])
            for n, o in enumerate((s.dwg, s.dwu))
        ]

    def y_out(s, q):
        k = lax.rem(q, 2)
        v = s.WGU.at[pl.ds(0, FF), pl.ds(pl.multiple_of(2 * XT + k * YT, YT), YT)]
        dst = s.dwd.at[:, pl.ds(pl.multiple_of(q * YT, YT), YT)]
        return v, pltpu.make_async_copy(v, dst, s.yo.at[k])

    def piece2(s, u):
        m = u - P2
        r = lax.rem(m, 3)

        @pl.when(m == 0)
        def _():
            s.x_tile(0)[1].start()
            s.y_tile(0)[1].start()

        @pl.when(r < 2)
        def _():
            q = (m // 3) * 2 + r
            pl.when(q + 1 < NX)(lambda: s.x_tile(q + 1)[1].start())
            tile, load = s.x_tile(q)
            load.wait()
            out, stores = s.x_out(q)

            @pl.when(q >= 2)
            def _():
                for c in s.x_out(q - 2)[1]:
                    c.wait()

            out[...] = dot(tile[...], s.DGU[...], 0, 0).astype(bf)
            for c in stores:
                c.start()

        @pl.when(r == 2)
        def _():
            q = m // 3
            pl.when(q + 1 < NY)(lambda: s.y_tile(q + 1)[1].start())
            tile, load = s.y_tile(q)
            load.wait()
            out, store = s.y_out(q)
            pl.when(q >= 2)(lambda: s.y_out(q - 2)[1].wait())
            out[...] = dot(s.HID[...], tile[...], 0, 0).astype(bf)
            store.start()

    def run(s):
        for c in s.group_loads(0):
            c.start()
        first, quarters = s.weights()
        first.start()
        for j in range(4):
            for c in quarters[j]:
                c.start()
        s.barrier()

        def iteration(u, _):
            pl.when((u <= P2) & (lax.rem(u, PPG) == 0))(lambda: s.before1(u))
            pl.when(u >= LEAD)(lambda: s.service(u - LEAD))
            pl.when(u < P2)(lambda: s.piece1(u))
            pl.when((u >= P2) & (u < P2 + PIECES2))(lambda: s.piece2(u))
            return 0

        lax.fori_loop(0, LEAD + STEPS, iteration, 0)
        s.finish()
        for q in (NX - 2, NX - 1):
            for c in s.x_out(q)[1]:
                c.wait()
        for q in (NY - 2, NY - 1):
            s.y_out(q)[1].wait()


def solution(mesh):
    def step(x, dy, gate, up, w_gate, w_up, w_down):
        shape = jax.ShapeDtypeStruct
        anywhere = pl.BlockSpec(memory_space=pl.ANY)
        dx, dw_gate, dw_up, dw_down, _, _ = pl.pallas_call(
            lambda *refs: Kernel(*refs).run(),
            out_shape=[
                shape((T_ROWS, D_MODEL), bf),
                shape((D_MODEL, FF), bf),
                shape((D_MODEL, FF), bf),
                shape((FF, D_MODEL), bf),
                shape((T_ROWS, HC), f32),
                shape((T_ROWS, HC), bf),
            ],
            in_specs=[anywhere] * 7,
            out_specs=[anywhere] * 6,
            scratch_shapes=list(SCRATCH.values()),
            compiler_params=pltpu.CompilerParams(
                collective_id=0, has_side_effects=True, vmem_limit_bytes=67043328
            ),
            name="mlp_backward",
        )(x, dy, gate, up, w_gate, w_up, w_down)
        return dx, dw_gate, dw_up, dw_down

    tokens, columns, rows = P("dp", None), P(None, "tp"), P("tp", None)
    return jax.shard_map(
        step,
        mesh=mesh,
        in_specs=(tokens, tokens, P("dp", "tp"), P("dp", "tp"), columns, columns, rows),
        out_specs=(tokens, P("dp", "tp"), P("dp", "tp"), P(("dp", "tp"), None)),
        check_vma=False,
    )
```

```python
import jax
import jax.numpy as jnp
from jax import lax
from jax.experimental import pallas as pl
from jax.experimental.pallas import tpu as pltpu
from jax.sharding import PartitionSpec as P

MESH = pl.DeviceIdType.MESH
bf, f32 = jnp.bfloat16, jnp.float32
DMA = pltpu.SemaphoreType.DMA
L = 128

T_ROWS, D_MODEL, FF = 2048, 5120, 896
HC = D_MODEL // 2
A, A2, BO, BT, MC = 6 * L, 3 * L, 12 * L, 2 * L, 14 * L

R, D = 32, 2
NB = T_ROWS // R
NS, NR, NH, W = 2 * D, 16, 4 * D + 4, 2
STEPS = NB + 8 * D
FILL, DRAIN = 4 * D, NB + 3 * D

G = 256
NG, BPG, PPG = T_ROWS // G, G // R, 6
LEAD = PPG
AHEAD = 2
DIRECT = 4
Q = D_MODEL // 4
F0 = 512
XT, YT = 256, 512
NX, NY = D_MODEL // XT, D_MODEL // YT
P2 = NG * PPG
WIDE = 4
PIECES2 = NX + 2 * NY - WIDE


def dot(a, b, ca, cb):
    return lax.dot_general(a, b, (((ca,), (cb,)), ((), ())), preferred_element_type=f32)


SCRATCH = dict(
    DGU=pltpu.VMEM((T_ROWS, 2 * FF), bf),
    HID=pltpu.VMEM((T_ROWS, FF), bf),
    POOL=pltpu.VMEM((T_ROWS, 2 * (XT + YT)), bf),
    GA=pltpu.VMEM((2, G, FF), bf),
    UP=pltpu.VMEM((2, G, FF), bf),
    PST=pltpu.VMEM((2, G, Q), bf),
    OST=pltpu.VMEM((2, G, Q), f32),
    H=pltpu.VMEM((NH, R, HC), f32),
    PT=pltpu.VMEM((4, R, HC), bf),
    F=pltpu.VMEM((NR, R, HC), bf),
    SR=pltpu.VMEM((NS, R, MC), bf),
    SL=pltpu.VMEM((NS, R, MC), bf),
    SY=pltpu.VMEM((NS, R, MC), bf),
    RR=pltpu.VMEM((NS, R, MC), bf),
    RL=pltpu.VMEM((NS, R, MC), bf),
    RY=pltpu.VMEM((NS, R, MC), bf),
    ss=DMA((3, NS)),
    rs=DMA((3, NS)),
    lh=DMA((4,)),
    lp=DMA((4,)),
    os=DMA((8,)),
    ds=DMA((8,)),
    dr=DMA((8,)),
    wd=DMA((4,)),
    wgu=DMA((4, 2)),
    ld=DMA((2, 6)),
    ps=DMA((2,)),
    pr=DMA((NG, 2)),
    ow=DMA((2,)),
    xl=DMA((2,)),
    yl=DMA((2,)),
)


OPERANDS = ("x", "dy", "gate", "up", "wg", "wu", "wd_h", "dx", "WGU", "WD", "own", "pt")


class Kernel:
    def __init__(s, *refs):
        s.__dict__.update(zip(OPERANDS + tuple(SCRATCH), refs, strict=True))
        i = lax.axis_index("tp")
        s.y, s.z, s.c = i // 8, lax.rem(i // 2, 4), lax.rem(i, 2)
        s.zm = 3 - s.z
        s.yid, s.cid = i + 8 - 16 * s.y, i + 1 - 2 * s.c
        s.rid, s.lid = jnp.minimum(i + 2, 15), jnp.maximum(i - 2, 0)
        s.has_r, s.has_l = s.z < 3, s.z > 0
        m = pl.multiple_of
        s.a0, s.o0 = m(s.y * A, L), m((1 - s.y) * A, L)
        s.a3, s.o3 = m(s.a0 + A2, L), m(s.o0 + A2, L)
        bz = BO + s.z * BT
        s.b_own, s.b_oth = m(bz + s.y * L, L), m(bz + (1 - s.y) * L, L)
        s.half = m(s.c * HC, HC)

    def barrier(s):
        b = pltpu.get_barrier_semaphore()

        def greet(d):
            pl.semaphore_signal(b, inc=1, device_id={"tp": d}, device_id_type=MESH)

        greet(s.yid)
        greet(s.cid)
        pl.when(s.has_r)(lambda: greet(s.rid))
        pl.when(s.has_l)(lambda: greet(s.lid))
        both = s.has_r & s.has_l
        pl.when(both)(lambda: pl.semaphore_wait(b, 4))
        pl.when(jnp.logical_not(both))(lambda: pl.semaphore_wait(b, 3))


    def loads(s, b):
        rows = pl.ds(pl.multiple_of(b * R, R), R)
        k = lax.rem(b, 4)
        return (
            pltpu.make_async_copy(s.own.at[rows], s.H.at[lax.rem(b, NH)], s.lh.at[k]),
            pltpu.make_async_copy(s.pt.at[rows], s.PT.at[k], s.lp.at[k]),
        )

    def message(s, link, t, kind):
        k = lax.rem(t, NS)
        lo, hi = (
            ((5 * L, MC), (0, 9 * L), (0, 7 * L)),
            ((0, MC),) * 3,
            ((0, 9 * L), (5 * L, MC), (7 * L, MC)),
        )[kind][link]
        src, dst = ((s.SR, s.RR), (s.SL, s.RL), (s.SY, s.RY))[link]
        at = (k, slice(None), pl.ds(lo, hi - lo))
        return pltpu.make_async_remote_copy(
            src_ref=src.at[at],
            dst_ref=dst.at[at],
            send_sem=s.ss.at[link, k],
            recv_sem=s.rs.at[link, k],
            device_id={"tp": (s.rid, s.lid, s.yid)[link]},
            device_id_type=MESH,
        )

    def messages(s, t, valid, do, right, left):
        def kind(k):
            do(s.message(2, t, k))
            pl.when(right)(lambda: do(s.message(0, t, k)))
            pl.when(left)(lambda: do(s.message(1, t, k)))

        pl.when(valid & (t < FILL))(lambda: kind(0))
        pl.when(valid & (t >= FILL) & (t < DRAIN))(lambda: kind(1))
        pl.when(valid & (t >= DRAIN) & (t < STEPS - D))(lambda: kind(2))

    def outs(s, b):
        k, q = lax.rem(b, NR), lax.rem(b, 8)
        dst = s.dx.at[pl.ds(pl.multiple_of(b * R, R), R), pl.ds(s.half, HC)]
        return (
            pltpu.make_async_copy(s.F.at[k], dst, s.os.at[q]),
            pltpu.make_async_remote_copy(
                src_ref=s.F.at[k],
                dst_ref=dst,
                send_sem=s.ds.at[q],
                recv_sem=s.dr.at[q],
                device_id={"tp": s.cid},
                device_id_type=MESH,
            ),
        )

    def wait_outs(s, b):
        for c in s.outs(b):
            c.wait()

    def chip_sum(s, b):
        own, partner = s.loads(b)
        pl.when(b >= DIRECT)(lambda: own.wait())
        partner.wait()
        k = lax.rem(b, NH)
        s.H[k] = s.H[k] + s.PT[lax.rem(b, 4)].astype(f32)

    def service(s, t):
        s.messages(t - D, t >= D, lambda c: c.wait_recv(), s.has_l, s.has_r)
        s.messages(t - NS, t >= NS, lambda c: c.wait_send(), s.has_r, s.has_l)

        def f(o):
            return lax.rem(t - o + 4 * NR, NR)

        def h(o):
            return lax.rem(t - o + 4 * NH, NH)

        H, F, z, zm = s.H, s.F, s.z, s.zm
        k, kr = lax.rem(t, NS), lax.rem(t + NS - D, NS)
        RY, RR, RL = s.RY.at[kr], s.RR.at[kr], s.RL.at[kr]
        SY, SR, SL = s.SY.at[k], s.SR.at[k], s.SL.at[k]

        own = (h(D), slice(None), pl.ds(s.a0, A))
        H[own] = H[own] + RY[:, 0 : 6 * L].astype(f32)
        rooted = H[h(4 * D), :, pl.ds(s.b_own, L)] + RY[:, 6 * L : 7 * L].astype(f32)
        F[f(4 * D), :, pl.ds(s.b_own, L)] = rooted.astype(bf)
        F[f(5 * D), :, pl.ds(s.b_oth, L)] = RY[:, 7 * L : 8 * L]
        F[f(5 * D + D * z), :, pl.ds(s.o0, A2)] = RY[:, 8 * L : 11 * L]
        F[f(5 * D + D * zm), :, pl.ds(s.o3, A2)] = RY[:, 11 * L : 14 * L]
        to_r = jnp.where(s.has_l, RR[:, 11 * L :].astype(f32), 0.0) + H[h(D + D * z), :, pl.ds(s.a3, A2)]
        to_l = jnp.where(s.has_r, RL[:, : 3 * L].astype(f32), 0.0) + H[h(D + D * zm), :, pl.ds(s.a0, A2)]
        to_r, to_l = to_r.astype(bf), to_l.astype(bf)
        f3 = jnp.where(s.has_r, RL[:, 11 * L :], to_r)
        f0 = jnp.where(s.has_l, RR[:, : 3 * L], to_l)
        F[f(4 * D + D * zm), :, pl.ds(s.a3, A2)] = f3
        F[f(4 * D + D * z), :, pl.ds(s.a0, A2)] = f0
        SR[:, 11 * L :], SR[:, : 3 * L] = to_r, f0
        SL[:, : 3 * L], SL[:, 11 * L :] = to_l, f3
        SY[:, 8 * L : 11 * L], SY[:, 11 * L :] = f0, f3
        hr, hl = h(D * z), h(D * zm)
        for q in range(4):
            b = pl.ds(BO + q * BT, BT)
            m = pl.ds(3 * L + q * BT, BT)
            rr, rl = RR[:, m], RL[:, m]
            sum_r = H[hr, :, b] + jnp.where(s.has_l, rr.astype(f32), 0.0)

            @pl.when(z == q)
            def _():
                H[hr, :, b] = sum_r

            sum_l = H[hl, :, b] + jnp.where(s.has_r, rl.astype(f32), 0.0)

            @pl.when(z == q)
            def _():
                H[hl, :, b] = sum_l

            fq = f(5 * D + D * jnp.abs(z - q))

            @pl.when(z > q)
            def _():
                F[fq, :, b] = rr

            @pl.when(z < q)
            def _():
                F[fq, :, b] = rl

            done = F[fq, :, b]
            SR[:, m] = jnp.where(z >= q, done, sum_r.astype(bf))
            SL[:, m] = jnp.where(z <= q, done, sum_l.astype(bf))
        SY[:, : 6 * L] = H[h(0), :, pl.ds(s.o0, A)].astype(bf)
        SY[:, 6 * L : 7 * L] = H[h(3 * D), :, pl.ds(s.b_oth, L)].astype(bf)
        SY[:, 7 * L : 8 * L] = F[f(4 * D), :, pl.ds(s.b_own, L)]
        s.messages(t, t >= 0, lambda c: c.start(), s.has_r, s.has_l)

        @pl.when(t >= 8 * D)
        def _():
            for c in s.outs(t - 8 * D):
                c.start()

        pl.when(t >= 8 * D + W)(lambda: s.wait_outs(t - 8 * D - W))

        @pl.when(t + AHEAD < NB)
        def _():
            b = t + AHEAD
            own, partner = s.loads(b)
            pl.when(lax.rem(b, BPG) == 0)(lambda: s.wait_partner(b // BPG))
            pl.when(b >= DIRECT)(lambda: own.start())
            partner.start()

        pl.when(t + 1 < NB)(lambda: s.chip_sum(t + 1))

    def finish(s):
        for b in range(NB - W, NB):
            s.wait_outs(b)
        for t in range(STEPS - D - NS + D, STEPS - D):
            s.message(2, t, 2).wait_send()
            pl.when(s.has_r)(lambda t=t: s.message(0, t, 2).wait_send())
            pl.when(s.has_l)(lambda t=t: s.message(1, t, 2).wait_send())


    def weights(s):
        def copy(src, dst, sem):
            return pltpu.make_async_copy(src, dst, sem)

        first, quarters = [], []
        for j in range(4):
            at = (slice(None), pl.ds(j * Q, Q))
            first.append(copy(s.wd_h.at[at], s.WD.at[at], s.wd.at[j]))
        for j in range(4):
            rows = pl.ds(s.quarter(j), Q)
            quarters.append(
                [
                    copy(w.at[rows], s.WGU.at[rows, pl.ds(n * FF, FF)], s.wgu.at[j, n])
                    for n, w in enumerate((s.wg, s.wu))
                ]
            )
        return first, quarters

    def quarter(s, j):
        mine = jnp.where(j < 2, 1 - s.c, s.c)
        return pl.multiple_of(mine * HC + lax.rem(j, 2) * Q, Q)

    def dy_part(s, g, j):
        return pl.ds(pl.multiple_of(lax.rem(g, 2) * 4 * G + j * G, G), G)

    def group_loads(s, g):
        k = lax.rem(g, 2)
        rows = pl.ds(pl.multiple_of(g * G, G), G)
        parts = [
            pltpu.make_async_copy(
                s.dy.at[rows, pl.ds(j * Q, Q)], s.POOL.at[s.dy_part(g, j), pl.ds(0, Q)], s.ld.at[k, j]
            )
            for j in range(4)
        ]
        return parts + [
            pltpu.make_async_copy(a.at[rows], v.at[k], s.ld.at[k, 4 + n])
            for n, (a, v) in enumerate(((s.gate, s.GA), (s.up, s.UP)))
        ]

    def to_partner(s, g, j):
        rows = pl.ds(pl.multiple_of(g * G, G), G)
        return pltpu.make_async_remote_copy(
            src_ref=s.PST.at[j],
            dst_ref=s.pt.at[rows, pl.ds(pl.multiple_of(j * Q, Q), Q)],
            send_sem=s.ps.at[j],
            recv_sem=s.pr.at[g, j],
            device_id={"tp": s.cid},
            device_id_type=MESH,
        )

    def to_own(s, g, j):
        rows = pl.ds(pl.multiple_of(g * G, G), G)
        dst = s.own.at[rows, pl.ds(pl.multiple_of(j * Q, Q), Q)]
        return pltpu.make_async_copy(s.OST.at[j], dst, s.ow.at[j])

    def wait_partner(s, g):
        for j in range(2):
            s.to_partner(g, j).wait_recv()

    def hidden(s, g, lo, hi):
        k = lax.rem(g, 2)
        rows = pl.ds(pl.multiple_of(g * G, G), G)
        d = sum(
            dot(s.POOL[s.dy_part(g, j), 0:Q], s.WD[lo:hi, j * Q : (j + 1) * Q], 1, 1)
            for j in range(4)
        )
        a, u = s.GA[k, :, lo:hi].astype(f32), s.UP[k, :, lo:hi].astype(f32)
        sig = jax.nn.sigmoid(a)
        silu = a * sig
        s.DGU[rows, lo:hi] = (d * u * (sig + silu * (1.0 - sig))).astype(bf)
        s.DGU[rows, FF + lo : FF + hi] = (d * silu).astype(bf)
        s.HID[rows, lo:hi] = (silu * u).astype(bf)

    def term(s, g, j):
        rows = pl.ds(pl.multiple_of(g * G, G), G)
        return dot(s.DGU[rows, :], s.WGU[pl.ds(s.quarter(j), Q), :], 1, 1)

    def before1(s, u):
        g, r = u // PPG, lax.rem(u, PPG)

        @pl.when(((r == 0) & (u >= 2 * PPG)) | (u == PPG + 2))
        def _():
            for j in range(2):
                s.to_partner(g - 1, j).wait_send()
                s.to_own(g - 1, j).wait()

        @pl.when(u == LEAD - 1)
        def _():
            s.wait_partner(0)
            for b in range(AHEAD):
                s.loads(b)[1].start()

        @pl.when(u == LEAD)
        def _():
            for b in range(DIRECT):
                for j in range(2):
                    s.H[b, :, j * Q : (j + 1) * Q] = s.OST[j, b * R : (b + 1) * R, :]
            s.chip_sum(jnp.int32(0))

        @pl.when((r == 0) & (g + 1 < NG))
        def _():
            for c in s.group_loads(g + 1):
                c.start()

    def piece1(s, u):
        g, r = u // PPG, lax.rem(u, PPG)
        first, quarters = s.weights()

        @pl.when(r == 0)
        def _():
            for n, c in enumerate(s.group_loads(g)):
                c.wait()
                if n < 4:

                    @pl.when(g == 0)
                    def _(n=n):
                        first[n].wait()
                        for c in quarters[n]:
                            c.start()

            s.hidden(g, 0, F0)

        pl.when(r == 1)(lambda: s.hidden(g, F0, FF))
        for j in range(4):

            @pl.when(u == 2 + j)
            def _(j=j):
                for c in quarters[j]:
                    c.wait()

        @pl.when((r == 2) | (r == 3))
        def _():
            j = r - 2
            s.PST[j] = s.term(g, j).astype(bf)
            s.to_partner(g, j).start()

        @pl.when(r >= 4)
        def _():
            j = r - 4
            s.OST[j] = s.term(g, r - 2)
            s.to_own(g, j).start()


    def x_tile(s, q):
        k = lax.rem(q, 2)
        v = s.POOL.at[:, pl.ds(pl.multiple_of(k * XT, XT), XT)]
        src = s.x.at[:, pl.ds(pl.multiple_of(q * XT, XT), XT)]
        return v, pltpu.make_async_copy(src, v, s.xl.at[k])

    def y_tile(s, q):
        k = lax.rem(q, 2)
        v = s.POOL.at[:, pl.ds(pl.multiple_of(2 * XT + k * YT, XT), YT)]
        src = s.dy.at[:, pl.ds(pl.multiple_of(q * YT, YT), YT)]
        return v, pltpu.make_async_copy(src, v, s.yl.at[k])

    def half_tile(s, q):
        k, n = lax.rem(q, 2), YT // 2
        v = s.POOL.at[:, pl.ds(pl.multiple_of(2 * XT + k * YT, XT), n)]
        src = s.dy.at[:, pl.ds(pl.multiple_of(WIDE * YT + q * n, n), n)]
        return v, pltpu.make_async_copy(src, v, s.yl.at[k])

    def piece2(s, u):
        m = u - P2

        @pl.when(m == 0)
        def _():
            s.x_tile(0)[1].start()
            s.y_tile(0)[1].start()

        @pl.when(m < NX)
        def _():
            pl.when(m + 1 < NX)(lambda: s.x_tile(m + 1)[1].start())
            tile, load = s.x_tile(m)
            load.wait()
            rows = pl.ds(pl.multiple_of(m * XT, XT), XT)
            s.WGU[rows, :] = dot(tile[...], s.DGU[...], 0, 0).astype(bf)

        @pl.when((m >= NX) & (m < NX + WIDE))
        def _():
            q = m - NX
            pl.when(q + 1 < WIDE)(lambda: s.y_tile(q + 1)[1].start())
            pl.when(q + 1 == WIDE)(lambda: s.half_tile(0)[1].start())
            tile, load = s.y_tile(q)
            load.wait()
            columns = pl.ds(pl.multiple_of(q * YT, YT), YT)
            s.WD[:, columns] = dot(s.HID[...], tile[...], 0, 0).astype(bf)

        @pl.when(m >= NX + WIDE)
        def _():
            q = m - NX - WIDE
            pl.when(m + 1 < PIECES2)(lambda: s.half_tile(q + 1)[1].start())
            tile, load = s.half_tile(q)
            load.wait()
            n = YT // 2
            columns = pl.ds(pl.multiple_of(WIDE * YT + q * n, n), n)
            s.WD[:, columns] = dot(s.HID[...], tile[...], 0, 0).astype(bf)

    def run(s):
        first, _ = s.weights()
        group = s.group_loads(0)
        for n in range(4):
            group[n].start()
            first[n].start()
        group[4].start()
        group[5].start()
        s.barrier()

        def iteration(u, _):
            pl.when(u <= P2)(lambda: s.before1(u))
            pl.when(u >= LEAD)(lambda: s.service(u - LEAD))
            pl.when(u < P2)(lambda: s.piece1(u))
            pl.when((u >= P2) & (u < P2 + PIECES2))(lambda: s.piece2(u))
            return 0

        lax.fori_loop(0, LEAD + STEPS, iteration, 0)
        s.finish()


XC, WC, YC = 16, 8, 8
SLOTS, LAG = 6, 2


def copy_out(dx, dwgu, dwd, dx_out, dwg_out, dwu_out, dwd_out, mid, rd, wr, gs, us, ys):
    def part(n, k, j):
        return pl.ds(j * (n // k), n // k)

    def read(j):
        at = part(T_ROWS, XC, j)
        return pltpu.make_async_copy(dx.at[at], mid.at[j % SLOTS], rd.at[j])

    def write(j):
        at = part(T_ROWS, XC, j)
        return pltpu.make_async_copy(mid.at[j % SLOTS], dx_out.at[at], wr.at[j])

    rest = []
    for j in range(WC):
        at = part(D_MODEL, WC, j)
        rest.append(pltpu.make_async_copy(dwgu.at[at, pl.ds(0, FF)], dwg_out.at[at], gs.at[j]))
        rest.append(pltpu.make_async_copy(dwgu.at[at, pl.ds(FF, FF)], dwu_out.at[at], us.at[j]))
        at = part(FF, YC, j)
        rest.append(pltpu.make_async_copy(dwd.at[at], dwd_out.at[at], ys.at[j]))
    for j in range(SLOTS):
        read(j).start()
    n = 0
    for j in range(XC):
        read(j).wait()
        write(j).start()
        for c in rest[n : (j + 1) * len(rest) // XC]:
            c.start()
        n = (j + 1) * len(rest) // XC
        if j >= LAG and j - LAG + SLOTS < XC:
            write(j - LAG).wait()
            read(j - LAG + SLOTS).start()
    for c in rest:
        c.wait()
    for j in range(XC - SLOTS, XC):
        write(j).wait()


def solution(mesh):
    def step(x, dy, gate, up, w_gate, w_up, w_down):
        shape = jax.ShapeDtypeStruct
        anywhere = pl.BlockSpec(memory_space=pl.ANY)
        vmem = pl.BlockSpec(memory_space=pltpu.VMEM)
        dx, dw_gu, dw_down, _, _ = pl.pallas_call(
            lambda *refs: Kernel(*refs).run(),
            out_shape=[
                shape((T_ROWS, D_MODEL), bf),
                pltpu.VMEM((D_MODEL, 2 * FF), bf),
                pltpu.VMEM((FF, D_MODEL), bf),
                shape((T_ROWS, HC), f32),
                shape((T_ROWS, HC), bf),
            ],
            in_specs=[anywhere] * 7,
            out_specs=[anywhere, vmem, vmem, anywhere, anywhere],
            scratch_shapes=list(SCRATCH.values()),
            compiler_params=pltpu.CompilerParams(
                collective_id=0, has_side_effects=True, vmem_limit_bytes=37 << 20
            ),
            name="mlp_backward",
        )(x, dy, gate, up, w_gate, w_up, w_down)
        return pl.pallas_call(
            copy_out,
            out_shape=[
                shape((T_ROWS, D_MODEL), bf),
                shape((D_MODEL, FF), bf),
                shape((D_MODEL, FF), bf),
                shape((FF, D_MODEL), bf),
            ],
            in_specs=[anywhere, vmem, vmem],
            out_specs=[anywhere] * 4,
            scratch_shapes=[
                pltpu.VMEM((SLOTS, T_ROWS // XC, D_MODEL), bf),
                DMA((XC,)),
                DMA((XC,)),
                DMA((WC,)),
                DMA((WC,)),
                DMA((YC,)),
            ],
            compiler_params=pltpu.CompilerParams(vmem_limit_bytes=8 << 20),
            name="copy_out",
        )(dx, dw_gu, dw_down)

    tokens, columns, rows = P("dp", None), P(None, "tp"), P("tp", None)
    return jax.shard_map(
        step,
        mesh=mesh,
        in_specs=(tokens, tokens, P("dp", "tp"), P("dp", "tp"), columns, columns, rows),
        out_specs=(tokens, P("dp", "tp"), P("dp", "tp"), P(("dp", "tp"), None)),
        check_vma=False,
    )
```

```python
import jax
import jax.numpy as jnp
from jax import lax
from jax.experimental import pallas as pl
from jax.experimental.pallas import tpu as pltpu
from jax.sharding import PartitionSpec as P

MESH = pl.DeviceIdType.MESH
bf, f32 = jnp.bfloat16, jnp.float32
DMA = pltpu.SemaphoreType.DMA
L = 128

T_ROWS, D_MODEL, FF = 2048, 5120, 896
HC = D_MODEL // 2
A, A2, BO, BT, MC = 6 * L, 3 * L, 12 * L, 2 * L, 14 * L

R, D = 32, 2
NB = T_ROWS // R
NS, NR, NH, W = 2 * D, 16, 4 * D + 4, 2
STEPS = NB + 8 * D
FILL, DRAIN = 4 * D, NB + 3 * D

G = 256
NG, BPG, PPG = T_ROWS // G, G // R, 6
LEAD = PPG
AHEAD = 2
DIRECT = 4
Q = D_MODEL // 4
F0 = 512
XT, YT = 256, 512
NX, NY = D_MODEL // XT, D_MODEL // YT
P2 = NG * PPG
WIDE = 4
PIECES2 = NX + 2 * NY - WIDE


def dot(a, b, ca, cb):
    return lax.dot_general(a, b, (((ca,), (cb,)), ((), ())), preferred_element_type=f32)


SCRATCH = dict(
    DGU=pltpu.VMEM((T_ROWS, 2 * FF), bf),
    HID=pltpu.VMEM((T_ROWS, FF), bf),
    POOL=pltpu.VMEM((T_ROWS, 2 * (XT + YT)), bf),
    GA=pltpu.VMEM((2, G, FF), bf),
    UP=pltpu.VMEM((2, G, FF), bf),
    PST=pltpu.VMEM((2, G, Q), bf),
    OST=pltpu.VMEM((2, G, Q), f32),
    H=pltpu.VMEM((NH, R, HC), f32),
    PT=pltpu.VMEM((4, R, HC), bf),
    F=pltpu.VMEM((NR, R, HC), bf),
    SR=pltpu.VMEM((NS, R, MC), bf),
    SL=pltpu.VMEM((NS, R, MC), bf),
    SY=pltpu.VMEM((NS, R, MC), bf),
    RR=pltpu.VMEM((NS, R, MC), bf),
    RL=pltpu.VMEM((NS, R, MC), bf),
    RY=pltpu.VMEM((NS, R, MC), bf),
    ss=DMA((3, NS)),
    rs=DMA((3, NS)),
    lh=DMA((4,)),
    lp=DMA((4,)),
    os=DMA((8,)),
    ds=DMA((8,)),
    dr=DMA((8,)),
    wd=DMA((4,)),
    wgu=DMA((4, 2)),
    ld=DMA((2, 6)),
    ps=DMA((2,)),
    pr=DMA((NG, 2)),
    ow=DMA((2,)),
    xl=DMA((2,)),
    yl=DMA((2,)),
)


OPERANDS = ("x", "dy", "gate", "up", "wg", "wu", "wd_h", "dx", "WGU", "WD", "own", "pt")


class Kernel:
    def __init__(s, *refs):
        s.__dict__.update(zip(OPERANDS + tuple(SCRATCH), refs, strict=True))
        i = lax.axis_index("tp")
        s.y, s.z, s.c = i // 8, lax.rem(i // 2, 4), lax.rem(i, 2)
        s.zm = 3 - s.z
        s.yid, s.cid = i + 8 - 16 * s.y, i + 1 - 2 * s.c
        s.rid, s.lid = jnp.minimum(i + 2, 15), jnp.maximum(i - 2, 0)
        s.has_r, s.has_l = s.z < 3, s.z > 0
        m = pl.multiple_of
        s.a0, s.o0 = m(s.y * A, L), m((1 - s.y) * A, L)
        s.a3, s.o3 = m(s.a0 + A2, L), m(s.o0 + A2, L)
        s.bz = m(BO + s.z * BT, L)
        s.b_own, s.b_oth = m(s.bz + s.y * L, L), m(s.bz + (1 - s.y) * L, L)
        s.half = m(s.c * HC, HC)

    def barrier(s):
        b = pltpu.get_barrier_semaphore()

        def greet(d):
            pl.semaphore_signal(b, inc=1, device_id={"tp": d}, device_id_type=MESH)

        greet(s.yid)
        greet(s.cid)
        pl.when(s.has_r)(lambda: greet(s.rid))
        pl.when(s.has_l)(lambda: greet(s.lid))
        both = s.has_r & s.has_l
        pl.when(both)(lambda: pl.semaphore_wait(b, 4))
        pl.when(jnp.logical_not(both))(lambda: pl.semaphore_wait(b, 3))


    def loads(s, b):
        rows = pl.ds(pl.multiple_of(b * R, R), R)
        k = lax.rem(b, 4)
        return (
            pltpu.make_async_copy(s.own.at[rows], s.H.at[lax.rem(b, NH)], s.lh.at[k]),
            pltpu.make_async_copy(s.pt.at[rows], s.PT.at[k], s.lp.at[k]),
        )

    def message(s, link, t, full):
        k = lax.rem(t, NS)
        src, dst = ((s.SR, s.RR), (s.SL, s.RL), (s.SY, s.RY))[link]
        at = k
        if not full:
            sums, results = ((5 * L, 0), (0, 5 * L), (0, 7 * L))[link]
            lo = pl.multiple_of(jnp.where(t < FILL, sums, results), L)
            at = (k, slice(None), pl.ds(lo, (9 * L, 9 * L, 7 * L)[link]))
        return pltpu.make_async_remote_copy(
            src_ref=src.at[at],
            dst_ref=dst.at[at],
            send_sem=s.ss.at[link, k],
            recv_sem=s.rs.at[link, k],
            device_id={"tp": (s.rid, s.lid, s.yid)[link]},
            device_id_type=MESH,
        )

    def messages(s, t, valid, do, *links):
        middle = (t >= FILL) & (t < DRAIN)

        def each(full):
            for link, there in links:
                pl.when(there)(lambda: do(s.message(link, t, full)))

        pl.when(valid & middle)(lambda: each(True))
        pl.when(valid & jnp.logical_not(middle) & (t < STEPS - D))(lambda: each(False))

    def outs(s, b):
        k, q = lax.rem(b, NR), lax.rem(b, 8)
        dst = s.dx.at[pl.ds(pl.multiple_of(b * R, R), R), pl.ds(s.half, HC)]
        return (
            pltpu.make_async_copy(s.F.at[k], dst, s.os.at[q]),
            pltpu.make_async_remote_copy(
                src_ref=s.F.at[k],
                dst_ref=dst,
                send_sem=s.ds.at[q],
                recv_sem=s.dr.at[q],
                device_id={"tp": s.cid},
                device_id_type=MESH,
            ),
        )

    def wait_outs(s, b):
        for c in s.outs(b):
            c.wait()

    def chip_sum(s, b):
        own, partner = s.loads(b)
        pl.when(b >= DIRECT)(lambda: own.wait())
        partner.wait()
        k = lax.rem(b, NH)
        s.H[k] = s.H[k] + s.PT[lax.rem(b, 4)].astype(f32)

    def service(s, t):
        always = t >= 0
        s.messages(t - NS, t >= NS, lambda c: c.wait_send(), (2, always), (0, s.has_r), (1, s.has_l))
        s.messages(t - D, t >= D, lambda c: c.wait_recv(), (2, always), (0, s.has_l), (1, s.has_r))

        def f(o):
            return lax.rem(t - o + 4 * NR, NR)

        def h(o):
            return lax.rem(t - o + 4 * NH, NH)

        H, F, z, zm = s.H, s.F, s.z, s.zm
        k, kr = lax.rem(t, NS), lax.rem(t + NS - D, NS)
        RY, RR, RL = s.RY.at[kr], s.RR.at[kr], s.RL.at[kr]
        SY, SR, SL = s.SY.at[k], s.SR.at[k], s.SL.at[k]

        own = (h(D), slice(None), pl.ds(s.a0, A))
        H[own] = H[own] + RY[:, 0 : 6 * L].astype(f32)
        rooted = H[h(4 * D), :, pl.ds(s.b_own, L)] + RY[:, 6 * L : 7 * L].astype(f32)
        F[f(4 * D), :, pl.ds(s.b_own, L)] = rooted.astype(bf)
        F[f(5 * D), :, pl.ds(s.b_oth, L)] = RY[:, 7 * L : 8 * L]
        F[f(5 * D + D * z), :, pl.ds(s.o0, A2)] = RY[:, 8 * L : 11 * L]
        F[f(5 * D + D * zm), :, pl.ds(s.o3, A2)] = RY[:, 11 * L : 14 * L]
        to_r = jnp.where(s.has_l, RR[:, 11 * L :].astype(f32), 0.0) + H[h(D + D * z), :, pl.ds(s.a3, A2)]
        to_l = jnp.where(s.has_r, RL[:, : 3 * L].astype(f32), 0.0) + H[h(D + D * zm), :, pl.ds(s.a0, A2)]
        to_r, to_l = to_r.astype(bf), to_l.astype(bf)
        f3 = jnp.where(s.has_r, RL[:, 11 * L :], to_r)
        f0 = jnp.where(s.has_l, RR[:, : 3 * L], to_l)
        F[f(4 * D + D * zm), :, pl.ds(s.a3, A2)] = f3
        F[f(4 * D + D * z), :, pl.ds(s.a0, A2)] = f0
        SR[:, 11 * L :], SR[:, : 3 * L] = to_r, f0
        SL[:, : 3 * L], SL[:, 11 * L :] = to_l, f3
        SY[:, 8 * L : 11 * L], SY[:, 11 * L :] = f0, f3
        hr, hl = h(D * z), h(D * zm)
        here, at = pl.ds(s.bz, BT), pl.ds(pl.multiple_of(s.bz - BO + A2, L), BT)
        H[hr, :, here] = H[hr, :, here] + jnp.where(s.has_l, RR[:, at].astype(f32), 0.0)
        H[hl, :, here] = H[hl, :, here] + jnp.where(s.has_r, RL[:, at].astype(f32), 0.0)
        for q in range(4):
            b = pl.ds(BO + q * BT, BT)
            m = pl.ds(A2 + q * BT, BT)
            fq = f(5 * D + D * jnp.abs(z - q))
            done = F[fq, :, b]
            if q < 3:
                done = jnp.where(z > q, RR[:, m], done)
            if q > 0:
                done = jnp.where(z < q, RL[:, m], done)
            F[fq, :, b] = done
            if q > 0:
                sum_r = H[hr, :, b] + jnp.where(s.has_l, RR[:, m].astype(f32), 0.0)
                SR[:, m] = jnp.where(z < q, sum_r.astype(bf), done)
            else:
                SR[:, m] = done
            if q < 3:
                sum_l = H[hl, :, b] + jnp.where(s.has_r, RL[:, m].astype(f32), 0.0)
                SL[:, m] = jnp.where(z > q, sum_l.astype(bf), done)
            else:
                SL[:, m] = done
        s.messages(t, always, lambda c: c.start(), (0, s.has_r), (1, s.has_l))
        SY[:, : 6 * L] = H[h(0), :, pl.ds(s.o0, A)].astype(bf)
        SY[:, 6 * L : 7 * L] = H[h(3 * D), :, pl.ds(s.b_oth, L)].astype(bf)
        SY[:, 7 * L : 8 * L] = F[f(4 * D), :, pl.ds(s.b_own, L)]
        s.messages(t, always, lambda c: c.start(), (2, always))

        @pl.when(t >= 8 * D)
        def _():
            for c in s.outs(t - 8 * D):
                c.start()

        pl.when(t >= 8 * D + W)(lambda: s.wait_outs(t - 8 * D - W))

        @pl.when(t + AHEAD < NB)
        def _():
            b = t + AHEAD
            own, partner = s.loads(b)
            pl.when(lax.rem(b, BPG) == 0)(lambda: s.wait_partner(b // BPG))
            pl.when(b >= DIRECT)(lambda: own.start())
            partner.start()

        pl.when(t + 1 < NB)(lambda: s.chip_sum(t + 1))

    def finish(s):
        for b in range(NB - W, NB):
            s.wait_outs(b)
        for t in range(STEPS - D - NS + D, STEPS - D):
            s.message(2, t, False).wait_send()
            pl.when(s.has_r)(lambda t=t: s.message(0, t, False).wait_send())
            pl.when(s.has_l)(lambda t=t: s.message(1, t, False).wait_send())


    def weights(s):
        def copy(src, dst, sem):
            return pltpu.make_async_copy(src, dst, sem)

        first, quarters = [], []
        for j in range(4):
            at = (slice(None), pl.ds(j * Q, Q))
            first.append(copy(s.wd_h.at[at], s.WD.at[at], s.wd.at[j]))
        for j in range(4):
            rows = pl.ds(s.quarter(j), Q)
            quarters.append(
                [
                    copy(w.at[rows], s.WGU.at[rows, pl.ds(n * FF, FF)], s.wgu.at[j, n])
                    for n, w in enumerate((s.wg, s.wu))
                ]
            )
        return first, quarters

    def quarter(s, j):
        mine = jnp.where(j < 2, 1 - s.c, s.c)
        return pl.multiple_of(mine * HC + lax.rem(j, 2) * Q, Q)

    def dy_part(s, g, j):
        return pl.ds(pl.multiple_of(lax.rem(g, 2) * 4 * G + j * G, G), G)

    def group_loads(s, g):
        k = lax.rem(g, 2)
        rows = pl.ds(pl.multiple_of(g * G, G), G)
        parts = [
            pltpu.make_async_copy(
                s.dy.at[rows, pl.ds(j * Q, Q)], s.POOL.at[s.dy_part(g, j), pl.ds(0, Q)], s.ld.at[k, j]
            )
            for j in range(4)
        ]
        return parts + [
            pltpu.make_async_copy(a.at[rows], v.at[k], s.ld.at[k, 4 + n])
            for n, (a, v) in enumerate(((s.gate, s.GA), (s.up, s.UP)))
        ]

    def to_partner(s, g, j):
        rows = pl.ds(pl.multiple_of(g * G, G), G)
        return pltpu.make_async_remote_copy(
            src_ref=s.PST.at[j],
            dst_ref=s.pt.at[rows, pl.ds(pl.multiple_of(j * Q, Q), Q)],
            send_sem=s.ps.at[j],
            recv_sem=s.pr.at[g, j],
            device_id={"tp": s.cid},
            device_id_type=MESH,
        )

    def to_own(s, g, j):
        rows = pl.ds(pl.multiple_of(g * G, G), G)
        dst = s.own.at[rows, pl.ds(pl.multiple_of(j * Q, Q), Q)]
        return pltpu.make_async_copy(s.OST.at[j], dst, s.ow.at[j])

    def wait_partner(s, g):
        for j in range(2):
            s.to_partner(g, j).wait_recv()

    def hidden(s, g, lo, hi, arrive=None):
        k = lax.rem(g, 2)
        rows = pl.ds(pl.multiple_of(g * G, G), G)
        d = 0.0
        for j in range(4):
            if arrive:
                arrive(j)
            d += dot(s.POOL[s.dy_part(g, j), 0:Q], s.WD[lo:hi, j * Q : (j + 1) * Q], 1, 1)
        a, u = s.GA[k, :, lo:hi].astype(f32), s.UP[k, :, lo:hi].astype(f32)
        sig = jax.nn.sigmoid(a)
        silu = a * sig
        s.DGU[rows, lo:hi] = (d * u * (sig + silu * (1.0 - sig))).astype(bf)
        s.DGU[rows, FF + lo : FF + hi] = (d * silu).astype(bf)
        s.HID[rows, lo:hi] = (silu * u).astype(bf)

    def term(s, g, j):
        rows = pl.ds(pl.multiple_of(g * G, G), G)
        return dot(s.DGU[rows, :], s.WGU[pl.ds(s.quarter(j), Q), :], 1, 1)

    def before1(s, u):
        g, r = u // PPG, lax.rem(u, PPG)

        @pl.when(((r == 0) & (u >= 2 * PPG)) | (u == PPG + 2))
        def _():
            for j in range(2):
                s.to_partner(g - 1, j).wait_send()
                s.to_own(g - 1, j).wait()

        @pl.when(u == LEAD - 1)
        def _():
            s.wait_partner(0)
            for b in range(AHEAD):
                s.loads(b)[1].start()

        @pl.when(u == LEAD)
        def _():
            for b in range(DIRECT):
                for j in range(2):
                    s.H[b, :, j * Q : (j + 1) * Q] = s.OST[j, b * R : (b + 1) * R, :]
            s.chip_sum(jnp.int32(0))

        @pl.when((r == 0) & (g + 1 < NG))
        def _():
            for c in s.group_loads(g + 1):
                c.start(priority=1)

    def piece1(s, u):
        g, r = u // PPG, lax.rem(u, PPG)
        first, quarters = s.weights()

        @pl.when(r == 0)
        def _():
            copies = s.group_loads(g)

            def arrive(n):
                copies[n].wait()

                @pl.when(g == 0)
                def _():
                    first[n].wait()
                    for c in quarters[n]:
                        c.start(priority=1)

                if n == 3:
                    copies[4].wait()
                    copies[5].wait()

            s.hidden(g, 0, F0, arrive)

        pl.when(r == 1)(lambda: s.hidden(g, F0, FF))
        for j in range(4):

            @pl.when(u == 2 + j)
            def _(j=j):
                for c in quarters[j]:
                    c.wait()

        @pl.when((r == 2) | (r == 3))
        def _():
            j = r - 2
            s.PST[j] = s.term(g, j).astype(bf)
            s.to_partner(g, j).start()

        @pl.when(r >= 4)
        def _():
            j = r - 4
            s.OST[j] = s.term(g, r - 2)
            s.to_own(g, j).start()


    def x_tile(s, q):
        k = lax.rem(q, 2)
        v = s.POOL.at[:, pl.ds(pl.multiple_of(k * XT, XT), XT)]
        src = s.x.at[:, pl.ds(pl.multiple_of(q * XT, XT), XT)]
        return v, pltpu.make_async_copy(src, v, s.xl.at[k])

    def y_tile(s, q):
        k = lax.rem(q, 2)
        v = s.POOL.at[:, pl.ds(pl.multiple_of(2 * XT + k * YT, XT), YT)]
        src = s.dy.at[:, pl.ds(pl.multiple_of(q * YT, YT), YT)]
        return v, pltpu.make_async_copy(src, v, s.yl.at[k])

    def half_tile(s, q):
        k, n = lax.rem(q, 2), YT // 2
        v = s.POOL.at[:, pl.ds(pl.multiple_of(2 * XT + k * YT, XT), n)]
        src = s.dy.at[:, pl.ds(pl.multiple_of(WIDE * YT + q * n, n), n)]
        return v, pltpu.make_async_copy(src, v, s.yl.at[k])

    def piece2(s, u):
        m = u - P2

        @pl.when(m < NX)
        def _():
            pl.when(m + 1 < NX)(lambda: s.x_tile(m + 1)[1].start(priority=1))
            tile, load = s.x_tile(m)
            load.wait()
            rows = pl.ds(pl.multiple_of(m * XT, XT), XT)
            s.WGU[rows, :] = dot(tile[...], s.DGU[...], 0, 0).astype(bf)

        @pl.when((m >= NX) & (m < NX + WIDE))
        def _():
            q = m - NX
            pl.when(q + 1 < WIDE)(lambda: s.y_tile(q + 1)[1].start(priority=1))
            pl.when(q + 1 == WIDE)(lambda: s.half_tile(0)[1].start(priority=1))
            tile, load = s.y_tile(q)
            load.wait()
            columns = pl.ds(pl.multiple_of(q * YT, YT), YT)
            s.WD[:, columns] = dot(s.HID[...], tile[...], 0, 0).astype(bf)

        @pl.when(m >= NX + WIDE)
        def _():
            q = m - NX - WIDE
            pl.when(m + 1 < PIECES2)(lambda: s.half_tile(q + 1)[1].start(priority=1))
            tile, load = s.half_tile(q)
            load.wait()
            n = YT // 2
            columns = pl.ds(pl.multiple_of(WIDE * YT + q * n, n), n)
            s.WD[:, columns] = dot(s.HID[...], tile[...], 0, 0).astype(bf)

    def run(s):
        first, _ = s.weights()
        group = s.group_loads(0)
        for n in range(4):
            group[n].start()
            first[n].start()
        group[4].start()
        group[5].start()
        s.barrier()

        def iteration(u, _):
            pl.when(u <= P2)(lambda: s.before1(u))
            pl.when(u >= LEAD)(lambda: s.service(u - LEAD))

            @pl.when(u == P2 - 3)
            def _():
                s.x_tile(0)[1].start(priority=1)
                s.y_tile(0)[1].start(priority=1)

            pl.when(u < P2)(lambda: s.piece1(u))
            pl.when((u >= P2) & (u < P2 + PIECES2))(lambda: s.piece2(u))
            return 0

        lax.fori_loop(0, LEAD + STEPS, iteration, 0)
        s.finish()


XC, WC, YC = 16, 8, 8
SLOTS, LAG = 6, 2


def copy_out(dx, dwgu, dwd, dx_out, dwg_out, dwu_out, dwd_out, mid, rd, wr, gs, us, ys):
    def part(n, k, j):
        return pl.ds(j * (n // k), n // k)

    def read(j):
        at = part(T_ROWS, XC, j)
        return pltpu.make_async_copy(dx.at[at], mid.at[j % SLOTS], rd.at[j])

    def write(j):
        at = part(T_ROWS, XC, j)
        return pltpu.make_async_copy(mid.at[j % SLOTS], dx_out.at[at], wr.at[j])

    rest = []
    for j in range(WC):
        at = part(D_MODEL, WC, j)
        rest.append(pltpu.make_async_copy(dwgu.at[at, pl.ds(0, FF)], dwg_out.at[at], gs.at[j]))
        rest.append(pltpu.make_async_copy(dwgu.at[at, pl.ds(FF, FF)], dwu_out.at[at], us.at[j]))
        at = part(FF, YC, j)
        rest.append(pltpu.make_async_copy(dwd.at[at], dwd_out.at[at], ys.at[j]))
    for j in range(SLOTS):
        read(j).start()
    n = 0
    for j in range(XC):
        read(j).wait()
        write(j).start()
        for c in rest[n : (j + 1) * len(rest) // XC]:
            c.start()
        n = (j + 1) * len(rest) // XC
        if j >= LAG and j - LAG + SLOTS < XC:
            write(j - LAG).wait()
            read(j - LAG + SLOTS).start()
    for c in rest:
        c.wait()
    for j in range(XC - SLOTS, XC):
        write(j).wait()


def solution(mesh):
    def step(x, dy, gate, up, w_gate, w_up, w_down):
        shape = jax.ShapeDtypeStruct
        anywhere = pl.BlockSpec(memory_space=pl.ANY)
        vmem = pl.BlockSpec(memory_space=pltpu.VMEM)
        dx, dw_gu, dw_down, _, _ = pl.pallas_call(
            lambda *refs: Kernel(*refs).run(),
            out_shape=[
                shape((T_ROWS, D_MODEL), bf),
                pltpu.VMEM((D_MODEL, 2 * FF), bf),
                pltpu.VMEM((FF, D_MODEL), bf),
                shape((T_ROWS, HC), f32),
                shape((T_ROWS, HC), bf),
            ],
            in_specs=[anywhere] * 7,
            out_specs=[anywhere, vmem, vmem, anywhere, anywhere],
            scratch_shapes=list(SCRATCH.values()),
            compiler_params=pltpu.CompilerParams(
                collective_id=0, has_side_effects=True, vmem_limit_bytes=37 << 20
            ),
            name="mlp_backward",
        )(x, dy, gate, up, w_gate, w_up, w_down)
        return pl.pallas_call(
            copy_out,
            out_shape=[
                shape((T_ROWS, D_MODEL), bf),
                shape((D_MODEL, FF), bf),
                shape((D_MODEL, FF), bf),
                shape((FF, D_MODEL), bf),
            ],
            in_specs=[anywhere, vmem, vmem],
            out_specs=[anywhere] * 4,
            scratch_shapes=[
                pltpu.VMEM((SLOTS, T_ROWS // XC, D_MODEL), bf),
                DMA((XC,)),
                DMA((XC,)),
                DMA((WC,)),
                DMA((WC,)),
                DMA((YC,)),
            ],
            compiler_params=pltpu.CompilerParams(vmem_limit_bytes=8 << 20),
            name="copy_out",
        )(dx, dw_gu, dw_down)

    tokens, columns, rows = P("dp", None), P(None, "tp"), P("tp", None)
    return jax.shard_map(
        step,
        mesh=mesh,
        in_specs=(tokens, tokens, P("dp", "tp"), P("dp", "tp"), columns, columns, rows),
        out_specs=(tokens, P("dp", "tp"), P("dp", "tp"), P(("dp", "tp"), None)),
        check_vma=False,
    )
```

```python
import jax
import jax.numpy as jnp
from jax import lax
from jax.experimental import pallas as pl
from jax.experimental.pallas import tpu as pltpu
from jax.sharding import PartitionSpec as P

MESH = pl.DeviceIdType.MESH
bf, f32 = jnp.bfloat16, jnp.float32
DMA = pltpu.SemaphoreType.DMA
L = 128

T_ROWS, D_MODEL, FF = 2048, 5120, 896
HC = D_MODEL // 2
A, A2, BO, BT, MC = 6 * L, 3 * L, 12 * L, 2 * L, 14 * L

R, D = 32, 2
NB = T_ROWS // R
NS, NR, NH, W = 2 * D, 16, 4 * D + 4, 2
STEPS = NB + 8 * D
FILL, DRAIN = 4 * D, NB + 3 * D

G = 256
NG, BPG, PPG = T_ROWS // G, G // R, 6
LEAD = PPG
AHEAD = 2
DIRECT = 4
Q = D_MODEL // 4
F0 = 512
XT, YT = 256, 512
NX, NY = D_MODEL // XT, D_MODEL // YT
P2 = NG * PPG
WIDE = 4
PIECES2 = NX + 2 * NY - WIDE


def dot(a, b, ca, cb):
    return lax.dot_general(a, b, (((ca,), (cb,)), ((), ())), preferred_element_type=f32)


SCRATCH = dict(
    DGU=pltpu.VMEM((T_ROWS, 2 * FF), bf),
    HID=pltpu.VMEM((T_ROWS, FF), bf),
    POOL=pltpu.VMEM((T_ROWS, 2 * (XT + YT)), bf),
    GA=pltpu.VMEM((2, G, FF), bf),
    UP=pltpu.VMEM((2, G, FF), bf),
    PST=pltpu.VMEM((2, G, Q), bf),
    OST=pltpu.VMEM((2, G, Q), f32),
    H=pltpu.VMEM((NH, R, HC), f32),
    PT=pltpu.VMEM((4, R, HC), bf),
    F=pltpu.VMEM((NR, R, HC), bf),
    SR=pltpu.VMEM((NS, R, MC), bf),
    SL=pltpu.VMEM((NS, R, MC), bf),
    SY=pltpu.VMEM((NS, R, MC), bf),
    RR=pltpu.VMEM((NS, R, MC), bf),
    RL=pltpu.VMEM((NS, R, MC), bf),
    RY=pltpu.VMEM((NS, R, MC), bf),
    ss=DMA((3, NS)),
    rs=DMA((3, NS)),
    lh=DMA((4,)),
    lp=DMA((4,)),
    os=DMA((8,)),
    ds=DMA((8,)),
    dr=DMA((8,)),
    wd=DMA((4,)),
    wgu=DMA((4, 2)),
    ld=DMA((2, 6)),
    ps=DMA((2,)),
    pr=DMA((NG, 2)),
    ow=DMA((2,)),
    xl=DMA((2,)),
    yl=DMA((2,)),
)


OPERANDS = ("x", "dy", "gate", "up", "wg", "wu", "wd_h", "dx", "WGU", "WD", "own", "pt")


class Kernel:
    def __init__(s, *refs):
        s.__dict__.update(zip(OPERANDS + tuple(SCRATCH), refs, strict=True))
        i = lax.axis_index("tp")
        s.y, s.z, s.c = i // 8, lax.rem(i // 2, 4), lax.rem(i, 2)
        s.zm = 3 - s.z
        other = 1 - 2 * s.c
        s.yid, s.cid = i + 8 - 16 * s.y + other, i + other
        s.rid, s.lid = jnp.minimum(i + 2 + other, 15), jnp.maximum(i - 2 + other, 0)
        s.side = lax.rem(s.c + s.y + s.z, 2)
        s.has_r, s.has_l = s.z < 3, s.z > 0
        m = pl.multiple_of
        s.a0, s.o0 = m(s.y * A, L), m((1 - s.y) * A, L)
        s.a3, s.o3 = m(s.a0 + A2, L), m(s.o0 + A2, L)
        s.bz = m(BO + s.z * BT, L)
        s.b_own, s.b_oth = m(s.bz + s.y * L, L), m(s.bz + (1 - s.y) * L, L)
        s.half = m(s.side * HC, HC)

    def barrier(s):
        b = pltpu.get_barrier_semaphore()

        def greet(d):
            pl.semaphore_signal(b, inc=1, device_id={"tp": d}, device_id_type=MESH)

        greet(s.yid)
        greet(s.cid)
        pl.when(s.has_r)(lambda: greet(s.rid))
        pl.when(s.has_l)(lambda: greet(s.lid))
        both = s.has_r & s.has_l
        pl.when(both)(lambda: pl.semaphore_wait(b, 4))
        pl.when(jnp.logical_not(both))(lambda: pl.semaphore_wait(b, 3))


    def loads(s, b):
        rows = pl.ds(pl.multiple_of(b * R, R), R)
        k = lax.rem(b, 4)
        return (
            pltpu.make_async_copy(s.own.at[rows], s.H.at[lax.rem(b, NH)], s.lh.at[k]),
            pltpu.make_async_copy(s.pt.at[rows], s.PT.at[k], s.lp.at[k]),
        )

    def message(s, link, t, full):
        k = lax.rem(t, NS)
        src, dst = ((s.SR, s.RR), (s.SL, s.RL), (s.SY, s.RY))[link]
        at = k
        if not full:
            sums, results = ((5 * L, 0), (0, 5 * L), (0, 7 * L))[link]
            lo = pl.multiple_of(jnp.where(t < FILL, sums, results), L)
            at = (k, slice(None), pl.ds(lo, (9 * L, 9 * L, 7 * L)[link]))
        return pltpu.make_async_remote_copy(
            src_ref=src.at[at],
            dst_ref=dst.at[at],
            send_sem=s.ss.at[link, k],
            recv_sem=s.rs.at[link, k],
            device_id={"tp": (s.rid, s.lid, s.yid)[link]},
            device_id_type=MESH,
        )

    def messages(s, t, valid, do, *links):
        middle = (t >= FILL) & (t < DRAIN)

        def each(full):
            for link, there in links:
                pl.when(there)(lambda: do(s.message(link, t, full)))

        pl.when(valid & middle)(lambda: each(True))
        pl.when(valid & jnp.logical_not(middle) & (t < STEPS - D))(lambda: each(False))

    def outs(s, b):
        k, q = lax.rem(b, NR), lax.rem(b, 8)
        dst = s.dx.at[pl.ds(pl.multiple_of(b * R, R), R), pl.ds(s.half, HC)]
        return (
            pltpu.make_async_copy(s.F.at[k], dst, s.os.at[q]),
            pltpu.make_async_remote_copy(
                src_ref=s.F.at[k],
                dst_ref=dst,
                send_sem=s.ds.at[q],
                recv_sem=s.dr.at[q],
                device_id={"tp": s.cid},
                device_id_type=MESH,
            ),
        )

    def wait_outs(s, b):
        for c in s.outs(b):
            c.wait()

    def chip_sum(s, b):
        own, partner = s.loads(b)
        pl.when(b >= DIRECT)(lambda: own.wait())
        partner.wait()
        k = lax.rem(b, NH)
        s.H[k] = s.H[k] + s.PT[lax.rem(b, 4)].astype(f32)

    def service(s, t):
        always = t >= 0
        s.messages(t - NS, t >= NS, lambda c: c.wait_send(), (2, always), (0, s.has_r), (1, s.has_l))
        s.messages(t - D, t >= D, lambda c: c.wait_recv(), (2, always), (0, s.has_l), (1, s.has_r))

        def f(o):
            return lax.rem(t - o + 4 * NR, NR)

        def h(o):
            return lax.rem(t - o + 4 * NH, NH)

        H, F, z, zm = s.H, s.F, s.z, s.zm
        k, kr = lax.rem(t, NS), lax.rem(t + NS - D, NS)
        RY, RR, RL = s.RY.at[kr], s.RR.at[kr], s.RL.at[kr]
        SY, SR, SL = s.SY.at[k], s.SR.at[k], s.SL.at[k]

        own = (h(D), slice(None), pl.ds(s.a0, A))
        H[own] = H[own] + RY[:, 0 : 6 * L].astype(f32)
        rooted = H[h(4 * D), :, pl.ds(s.b_own, L)] + RY[:, 6 * L : 7 * L].astype(f32)
        F[f(4 * D), :, pl.ds(s.b_own, L)] = rooted.astype(bf)
        F[f(5 * D), :, pl.ds(s.b_oth, L)] = RY[:, 7 * L : 8 * L]
        F[f(5 * D + D * z), :, pl.ds(s.o0, A2)] = RY[:, 8 * L : 11 * L]
        F[f(5 * D + D * zm), :, pl.ds(s.o3, A2)] = RY[:, 11 * L : 14 * L]
        to_r = jnp.where(s.has_l, RR[:, 11 * L :].astype(f32), 0.0) + H[h(D + D * z), :, pl.ds(s.a3, A2)]
        to_l = jnp.where(s.has_r, RL[:, : 3 * L].astype(f32), 0.0) + H[h(D + D * zm), :, pl.ds(s.a0, A2)]
        to_r, to_l = to_r.astype(bf), to_l.astype(bf)
        f3 = jnp.where(s.has_r, RL[:, 11 * L :], to_r)
        f0 = jnp.where(s.has_l, RR[:, : 3 * L], to_l)
        F[f(4 * D + D * zm), :, pl.ds(s.a3, A2)] = f3
        F[f(4 * D + D * z), :, pl.ds(s.a0, A2)] = f0
        SR[:, 11 * L :], SR[:, : 3 * L] = to_r, f0
        SL[:, : 3 * L], SL[:, 11 * L :] = to_l, f3
        SY[:, 8 * L : 11 * L], SY[:, 11 * L :] = f0, f3
        hr, hl = h(D * z), h(D * zm)
        here, at = pl.ds(s.bz, BT), pl.ds(pl.multiple_of(s.bz - BO + A2, L), BT)
        H[hr, :, here] = H[hr, :, here] + jnp.where(s.has_l, RR[:, at].astype(f32), 0.0)
        H[hl, :, here] = H[hl, :, here] + jnp.where(s.has_r, RL[:, at].astype(f32), 0.0)
        for q in range(4):
            b = pl.ds(BO + q * BT, BT)
            m = pl.ds(A2 + q * BT, BT)
            fq = f(5 * D + D * jnp.abs(z - q))
            done = F[fq, :, b]
            if q < 3:
                done = jnp.where(z > q, RR[:, m], done)
            if q > 0:
                done = jnp.where(z < q, RL[:, m], done)
            F[fq, :, b] = done
            if q > 0:
                sum_r = H[hr, :, b] + jnp.where(s.has_l, RR[:, m].astype(f32), 0.0)
                SR[:, m] = jnp.where(z < q, sum_r.astype(bf), done)
            else:
                SR[:, m] = done
            if q < 3:
                sum_l = H[hl, :, b] + jnp.where(s.has_r, RL[:, m].astype(f32), 0.0)
                SL[:, m] = jnp.where(z > q, sum_l.astype(bf), done)
            else:
                SL[:, m] = done
        s.messages(t, always, lambda c: c.start(), (0, s.has_r), (1, s.has_l))
        SY[:, : 6 * L] = H[h(0), :, pl.ds(s.o0, A)].astype(bf)
        SY[:, 6 * L : 7 * L] = H[h(3 * D), :, pl.ds(s.b_oth, L)].astype(bf)
        SY[:, 7 * L : 8 * L] = F[f(4 * D), :, pl.ds(s.b_own, L)]
        s.messages(t, always, lambda c: c.start(), (2, always))

        @pl.when(t >= 8 * D)
        def _():
            for c in s.outs(t - 8 * D):
                c.start()

        pl.when(t >= 8 * D + W)(lambda: s.wait_outs(t - 8 * D - W))

        @pl.when(t + AHEAD < NB)
        def _():
            b = t + AHEAD
            own, partner = s.loads(b)
            pl.when(lax.rem(b, BPG) == 0)(lambda: s.wait_partner(b // BPG))
            pl.when(b >= DIRECT)(lambda: own.start())
            partner.start()

        pl.when(t + 1 < NB)(lambda: s.chip_sum(t + 1))

    def finish(s):
        for b in range(NB - W, NB):
            s.wait_outs(b)
        for t in range(STEPS - D - NS + D, STEPS - D):
            s.message(2, t, False).wait_send()
            pl.when(s.has_r)(lambda t=t: s.message(0, t, False).wait_send())
            pl.when(s.has_l)(lambda t=t: s.message(1, t, False).wait_send())


    def weights(s):
        def copy(src, dst, sem):
            return pltpu.make_async_copy(src, dst, sem)

        first, quarters = [], []
        for j in range(4):
            at = (slice(None), pl.ds(j * Q, Q))
            first.append(copy(s.wd_h.at[at], s.WD.at[at], s.wd.at[j]))
        for j in range(4):
            rows = pl.ds(s.quarter(j), Q)
            quarters.append(
                [
                    copy(w.at[rows], s.WGU.at[rows, pl.ds(n * FF, FF)], s.wgu.at[j, n])
                    for n, w in enumerate((s.wg, s.wu))
                ]
            )
        return first, quarters

    def quarter(s, j):
        mine = jnp.where(j < 2, 1 - s.side, s.side)
        return pl.multiple_of(mine * HC + lax.rem(j, 2) * Q, Q)

    def dy_part(s, g, j):
        return pl.ds(pl.multiple_of(lax.rem(g, 2) * 4 * G + j * G, G), G)

    def group_loads(s, g):
        k = lax.rem(g, 2)
        rows = pl.ds(pl.multiple_of(g * G, G), G)
        parts = [
            pltpu.make_async_copy(
                s.dy.at[rows, pl.ds(j * Q, Q)], s.POOL.at[s.dy_part(g, j), pl.ds(0, Q)], s.ld.at[k, j]
            )
            for j in range(4)
        ]
        return parts + [
            pltpu.make_async_copy(a.at[rows], v.at[k], s.ld.at[k, 4 + n])
            for n, (a, v) in enumerate(((s.gate, s.GA), (s.up, s.UP)))
        ]

    def to_partner(s, g, j):
        rows = pl.ds(pl.multiple_of(g * G, G), G)
        return pltpu.make_async_remote_copy(
            src_ref=s.PST.at[j],
            dst_ref=s.pt.at[rows, pl.ds(pl.multiple_of(j * Q, Q), Q)],
            send_sem=s.ps.at[j],
            recv_sem=s.pr.at[g, j],
            device_id={"tp": s.cid},
            device_id_type=MESH,
        )

    def to_own(s, g, j):
        rows = pl.ds(pl.multiple_of(g * G, G), G)
        dst = s.own.at[rows, pl.ds(pl.multiple_of(j * Q, Q), Q)]
        return pltpu.make_async_copy(s.OST.at[j], dst, s.ow.at[j])

    def wait_partner(s, g):
        for j in range(2):
            s.to_partner(g, j).wait_recv()

    def hidden(s, g, lo, hi, arrive=None):
        k = lax.rem(g, 2)
        rows = pl.ds(pl.multiple_of(g * G, G), G)
        d = 0.0
        for j in range(4):
            if arrive:
                arrive(j)
            d += dot(s.POOL[s.dy_part(g, j), 0:Q], s.WD[lo:hi, j * Q : (j + 1) * Q], 1, 1)
        a, u = s.GA[k, :, lo:hi].astype(f32), s.UP[k, :, lo:hi].astype(f32)
        sig = jax.nn.sigmoid(a)
        silu = a * sig
        s.DGU[rows, lo:hi] = (d * u * (sig + silu * (1.0 - sig))).astype(bf)
        s.DGU[rows, FF + lo : FF + hi] = (d * silu).astype(bf)
        s.HID[rows, lo:hi] = (silu * u).astype(bf)

    def term(s, g, j):
        rows = pl.ds(pl.multiple_of(g * G, G), G)
        return dot(s.DGU[rows, :], s.WGU[pl.ds(s.quarter(j), Q), :], 1, 1)

    def before1(s, u):
        g, r = u // PPG, lax.rem(u, PPG)

        @pl.when(((r == 0) & (u >= 2 * PPG)) | (u == PPG + 2))
        def _():
            for j in range(2):
                s.to_partner(g - 1, j).wait_send()
                s.to_own(g - 1, j).wait()

        @pl.when(u == LEAD - 1)
        def _():
            s.wait_partner(0)
            for b in range(AHEAD):
                s.loads(b)[1].start()

        @pl.when(u == LEAD)
        def _():
            for b in range(DIRECT):
                for j in range(2):
                    s.H[b, :, j * Q : (j + 1) * Q] = s.OST[j, b * R : (b + 1) * R, :]
            s.chip_sum(jnp.int32(0))

        @pl.when((u == LEAD) & (s.side == 1))
        def _():
            pl.delay(700)

        @pl.when((r == 0) & (g + 1 < NG))
        def _():
            for c in s.group_loads(g + 1):
                c.start(priority=1)

    def piece1(s, u):
        g, r = u // PPG, lax.rem(u, PPG)
        first, quarters = s.weights()

        @pl.when(r == 0)
        def _():
            copies = s.group_loads(g)

            def arrive(n):
                copies[n].wait()

                @pl.when(g == 0)
                def _():
                    first[n].wait()
                    for c in quarters[n]:
                        c.start(priority=1)

                if n == 3:
                    copies[4].wait()
                    copies[5].wait()

            s.hidden(g, 0, F0, arrive)

        pl.when(r == 1)(lambda: s.hidden(g, F0, FF))
        for j in range(4):

            @pl.when(u == 2 + j)
            def _(j=j):
                for c in quarters[j]:
                    c.wait()

        @pl.when((r == 2) | (r == 3))
        def _():
            j = r - 2
            s.PST[j] = s.term(g, j).astype(bf)
            s.to_partner(g, j).start()

        @pl.when(r >= 4)
        def _():
            j = r - 4
            s.OST[j] = s.term(g, r - 2)
            s.to_own(g, j).start()


    def x_tile(s, q):
        k = lax.rem(q, 2)
        v = s.POOL.at[:, pl.ds(pl.multiple_of(k * XT, XT), XT)]
        src = s.x.at[:, pl.ds(pl.multiple_of(q * XT, XT), XT)]
        return v, pltpu.make_async_copy(src, v, s.xl.at[k])

    def y_tile(s, q):
        k = lax.rem(q, 2)
        v = s.POOL.at[:, pl.ds(pl.multiple_of(2 * XT + k * YT, XT), YT)]
        src = s.dy.at[:, pl.ds(pl.multiple_of(q * YT, YT), YT)]
        return v, pltpu.make_async_copy(src, v, s.yl.at[k])

    def half_tile(s, q):
        k, n = lax.rem(q, 2), YT // 2
        v = s.POOL.at[:, pl.ds(pl.multiple_of(2 * XT + k * YT, XT), n)]
        src = s.dy.at[:, pl.ds(pl.multiple_of(WIDE * YT + q * n, n), n)]
        return v, pltpu.make_async_copy(src, v, s.yl.at[k])

    def piece2(s, u):
        m = u - P2

        @pl.when(m < NX)
        def _():
            pl.when(m + 1 < NX)(lambda: s.x_tile(m + 1)[1].start(priority=1))
            tile, load = s.x_tile(m)
            load.wait()
            rows = pl.ds(pl.multiple_of(m * XT, XT), XT)
            s.WGU[rows, :] = dot(tile[...], s.DGU[...], 0, 0).astype(bf)

        @pl.when((m >= NX) & (m < NX + WIDE))
        def _():
            q = m - NX
            pl.when(q + 1 < WIDE)(lambda: s.y_tile(q + 1)[1].start(priority=1))
            pl.when(q + 1 == WIDE)(lambda: s.half_tile(0)[1].start(priority=1))
            tile, load = s.y_tile(q)
            load.wait()
            columns = pl.ds(pl.multiple_of(q * YT, YT), YT)
            s.WD[:, columns] = dot(s.HID[...], tile[...], 0, 0).astype(bf)

        @pl.when(m >= NX + WIDE)
        def _():
            q = m - NX - WIDE
            pl.when(m + 1 < PIECES2)(lambda: s.half_tile(q + 1)[1].start(priority=1))
            tile, load = s.half_tile(q)
            load.wait()
            n = YT // 2
            columns = pl.ds(pl.multiple_of(WIDE * YT + q * n, n), n)
            s.WD[:, columns] = dot(s.HID[...], tile[...], 0, 0).astype(bf)

    def run(s):
        first, _ = s.weights()
        group = s.group_loads(0)
        for n in range(4):
            group[n].start()
            first[n].start()
        group[4].start()
        group[5].start()
        s.barrier()

        def iteration(u, _):
            pl.when(u <= P2)(lambda: s.before1(u))
            pl.when(u >= LEAD)(lambda: s.service(u - LEAD))

            @pl.when(u == P2 - 3)
            def _():
                s.x_tile(0)[1].start(priority=1)
                s.y_tile(0)[1].start(priority=1)

            pl.when(u < P2)(lambda: s.piece1(u))
            pl.when((u >= P2) & (u < P2 + PIECES2))(lambda: s.piece2(u))
            return 0

        lax.fori_loop(0, LEAD + STEPS, iteration, 0)
        s.finish()


XC, WC, YC = 16, 8, 8
SLOTS, LAG = 6, 2


def copy_out(dx, dwgu, dwd, dx_out, dwg_out, dwu_out, dwd_out, mid, rd, wr, gs, us, ys):
    def part(n, k, j):
        return pl.ds(j * (n // k), n // k)

    def read(j):
        at = part(T_ROWS, XC, j)
        return pltpu.make_async_copy(dx.at[at], mid.at[j % SLOTS], rd.at[j])

    def write(j):
        at = part(T_ROWS, XC, j)
        return pltpu.make_async_copy(mid.at[j % SLOTS], dx_out.at[at], wr.at[j])

    rest = []
    for j in range(WC):
        at = part(D_MODEL, WC, j)
        rest.append(pltpu.make_async_copy(dwgu.at[at, pl.ds(0, FF)], dwg_out.at[at], gs.at[j]))
        rest.append(pltpu.make_async_copy(dwgu.at[at, pl.ds(FF, FF)], dwu_out.at[at], us.at[j]))
        at = part(FF, YC, j)
        rest.append(pltpu.make_async_copy(dwd.at[at], dwd_out.at[at], ys.at[j]))
    for j in range(SLOTS):
        read(j).start()
    n = 0
    for j in range(XC):
        read(j).wait()
        write(j).start()
        for c in rest[n : (j + 1) * len(rest) // XC]:
            c.start()
        n = (j + 1) * len(rest) // XC
        if j >= LAG and j - LAG + SLOTS < XC:
            write(j - LAG).wait()
            read(j - LAG + SLOTS).start()
    for c in rest:
        c.wait()
    for j in range(XC - SLOTS, XC):
        write(j).wait()


def solution(mesh):
    def step(x, dy, gate, up, w_gate, w_up, w_down):
        shape = jax.ShapeDtypeStruct
        anywhere = pl.BlockSpec(memory_space=pl.ANY)
        vmem = pl.BlockSpec(memory_space=pltpu.VMEM)
        dx, dw_gu, dw_down, _, _ = pl.pallas_call(
            lambda *refs: Kernel(*refs).run(),
            out_shape=[
                shape((T_ROWS, D_MODEL), bf),
                pltpu.VMEM((D_MODEL, 2 * FF), bf),
                pltpu.VMEM((FF, D_MODEL), bf),
                shape((T_ROWS, HC), f32),
                shape((T_ROWS, HC), bf),
            ],
            in_specs=[anywhere] * 7,
            out_specs=[anywhere, vmem, vmem, anywhere, anywhere],
            scratch_shapes=list(SCRATCH.values()),
            compiler_params=pltpu.CompilerParams(
                collective_id=0, has_side_effects=True, vmem_limit_bytes=37 << 20
            ),
            name="mlp_backward",
        )(x, dy, gate, up, w_gate, w_up, w_down)
        return pl.pallas_call(
            copy_out,
            out_shape=[
                shape((T_ROWS, D_MODEL), bf),
                shape((D_MODEL, FF), bf),
                shape((D_MODEL, FF), bf),
                shape((FF, D_MODEL), bf),
            ],
            in_specs=[anywhere, vmem, vmem],
            out_specs=[anywhere] * 4,
            scratch_shapes=[
                pltpu.VMEM((SLOTS, T_ROWS // XC, D_MODEL), bf),
                DMA((XC,)),
                DMA((XC,)),
                DMA((WC,)),
                DMA((WC,)),
                DMA((YC,)),
            ],
            compiler_params=pltpu.CompilerParams(vmem_limit_bytes=8 << 20),
            name="copy_out",
        )(dx, dw_gu, dw_down)

    tokens, columns, rows = P("dp", None), P(None, "tp"), P("tp", None)
    return jax.shard_map(
        step,
        mesh=mesh,
        in_specs=(tokens, tokens, P("dp", "tp"), P("dp", "tp"), columns, columns, rows),
        out_specs=(tokens, P("dp", "tp"), P("dp", "tp"), P(("dp", "tp"), None)),
        check_vma=False,
    )
```

```python
import jax
import jax.numpy as jnp
from jax import lax
from jax.experimental import pallas as pl
from jax.experimental.pallas import tpu as pltpu
from jax.sharding import PartitionSpec as P

MESH = pl.DeviceIdType.MESH
bf, f32 = jnp.bfloat16, jnp.float32
DMA = pltpu.SemaphoreType.DMA
L = 128

T_ROWS, D_MODEL, FF = 2048, 5120, 896
HC = D_MODEL // 2
A, A2, BO, BT, MC = 6 * L, 3 * L, 12 * L, 2 * L, 14 * L

R, D = 32, 2
NB = T_ROWS // R
NS, NR, NH, W = 2 * D, 16, 4 * D + 4, 2
STEPS = NB + 8 * D
FILL, DRAIN = 4 * D, NB + 3 * D

G = 256
NG, BPG, PPG = T_ROWS // G, G // R, 6
LEAD = PPG
AHEAD = 2
DIRECT = 4
Q = D_MODEL // 4
F0 = 512
XT, YT = 256, 512
NX, NY = D_MODEL // XT, D_MODEL // YT
P2 = NG * PPG
WIDE = 4
PIECES2 = NX + 2 * NY - WIDE


def dot(a, b, ca, cb):
    return lax.dot_general(a, b, (((ca,), (cb,)), ((), ())), preferred_element_type=f32)


SCRATCH = dict(
    DGU=pltpu.VMEM((T_ROWS, 2 * FF), bf),
    HID=pltpu.VMEM((T_ROWS, FF), bf),
    POOL=pltpu.VMEM((T_ROWS, 2 * (XT + YT)), bf),
    GA=pltpu.VMEM((2, G, FF), bf),
    UP=pltpu.VMEM((2, G, FF), bf),
    PST=pltpu.VMEM((2, G, Q), bf),
    OST=pltpu.VMEM((2, G, Q), f32),
    H=pltpu.VMEM((NH, R, HC), f32),
    PT=pltpu.VMEM((4, R, HC), bf),
    F=pltpu.VMEM((NR, R, HC), bf),
    SR=pltpu.VMEM((NS, R, MC), bf),
    SL=pltpu.VMEM((NS, R, MC), bf),
    SY=pltpu.VMEM((NS, R, MC), bf),
    RR=pltpu.VMEM((NS, R, MC), bf),
    RL=pltpu.VMEM((NS, R, MC), bf),
    RY=pltpu.VMEM((NS, R, MC), bf),
    ss=DMA((3, NS)),
    rs=DMA((3, NS)),
    lh=DMA((4,)),
    lp=DMA((4,)),
    os=DMA((8,)),
    ds=DMA((8,)),
    dr=DMA((8,)),
    wd=DMA((4,)),
    wgu=DMA((4, 2)),
    ld=DMA((2, 6)),
    ps=DMA((2,)),
    pr=DMA((NG, 2)),
    ow=DMA((2,)),
    xl=DMA((2,)),
    yl=DMA((2,)),
)


OPERANDS = ("x", "dy", "gate", "up", "wg", "wu", "wd_h", "dx", "WGU", "WD", "own", "pt")


class Kernel:
    def __init__(s, *refs):
        s.__dict__.update(zip(OPERANDS + tuple(SCRATCH), refs, strict=True))
        i = lax.axis_index("tp")
        s.y, s.z, s.c = i // 8, lax.rem(i // 2, 4), lax.rem(i, 2)
        s.zm = 3 - s.z
        other = 1 - 2 * s.c
        s.yid, s.cid = i + 8 - 16 * s.y + other, i + other
        s.rid, s.lid = jnp.minimum(i + 2 + other, 15), jnp.maximum(i - 2 + other, 0)
        s.side = lax.rem(s.c + s.y + s.z, 2)
        s.has_r, s.has_l = s.z < 3, s.z > 0
        m = pl.multiple_of
        s.a0, s.o0 = m(s.y * A, L), m((1 - s.y) * A, L)
        s.a3, s.o3 = m(s.a0 + A2, L), m(s.o0 + A2, L)
        s.bz = m(BO + s.z * BT, L)
        s.b_own, s.b_oth = m(s.bz + s.y * L, L), m(s.bz + (1 - s.y) * L, L)
        s.half = m(s.side * HC, HC)

    def barrier(s):
        b = pltpu.get_barrier_semaphore()

        def greet(d):
            pl.semaphore_signal(b, inc=1, device_id={"tp": d}, device_id_type=MESH)

        greet(s.yid)
        greet(s.cid)
        pl.when(s.has_r)(lambda: greet(s.rid))
        pl.when(s.has_l)(lambda: greet(s.lid))
        both = s.has_r & s.has_l
        pl.when(both)(lambda: pl.semaphore_wait(b, 4))
        pl.when(jnp.logical_not(both))(lambda: pl.semaphore_wait(b, 3))


    def loads(s, b):
        rows = pl.ds(pl.multiple_of(b * R, R), R)
        k = lax.rem(b, 4)
        return (
            pltpu.make_async_copy(s.own.at[rows], s.H.at[lax.rem(b, NH)], s.lh.at[k]),
            pltpu.make_async_copy(s.pt.at[rows], s.PT.at[k], s.lp.at[k]),
        )

    def message(s, link, t, full):
        k = lax.rem(t, NS)
        src, dst = ((s.SR, s.RR), (s.SL, s.RL), (s.SY, s.RY))[link]
        at = k
        if not full:
            sums, results = ((5 * L, 0), (0, 5 * L), (0, 7 * L))[link]
            lo = pl.multiple_of(jnp.where(t < FILL, sums, results), L)
            at = (k, slice(None), pl.ds(lo, (9 * L, 9 * L, 7 * L)[link]))
        return pltpu.make_async_remote_copy(
            src_ref=src.at[at],
            dst_ref=dst.at[at],
            send_sem=s.ss.at[link, k],
            recv_sem=s.rs.at[link, k],
            device_id={"tp": (s.rid, s.lid, s.yid)[link]},
            device_id_type=MESH,
        )

    def messages(s, t, valid, do, *links):
        middle = (t >= FILL) & (t < DRAIN)

        def each(full):
            for link, there in links:
                pl.when(there)(lambda: do(s.message(link, t, full)))

        pl.when(valid & middle)(lambda: each(True))
        pl.when(valid & jnp.logical_not(middle) & (t < STEPS - D))(lambda: each(False))

    def outs(s, b):
        k, q = lax.rem(b, NR), lax.rem(b, 8)
        dst = s.dx.at[pl.ds(pl.multiple_of(b * R, R), R), pl.ds(s.half, HC)]
        return (
            pltpu.make_async_copy(s.F.at[k], dst, s.os.at[q]),
            pltpu.make_async_remote_copy(
                src_ref=s.F.at[k],
                dst_ref=dst,
                send_sem=s.ds.at[q],
                recv_sem=s.dr.at[q],
                device_id={"tp": s.cid},
                device_id_type=MESH,
            ),
        )

    def wait_outs(s, b):
        for c in s.outs(b):
            c.wait()

    def chip_sum(s, b):
        own, partner = s.loads(b)
        pl.when(b >= DIRECT)(lambda: own.wait())
        partner.wait()
        k = lax.rem(b, NH)
        s.H[k] = s.H[k] + s.PT[lax.rem(b, 4)].astype(f32)

    def service(s, t):
        always = t >= 0
        s.messages(t - NS, t >= NS, lambda c: c.wait_send(), (2, always), (0, s.has_r), (1, s.has_l))
        s.messages(t - D, t >= D, lambda c: c.wait_recv(), (2, always), (0, s.has_l), (1, s.has_r))

        def f(o):
            return lax.rem(t - o + 4 * NR, NR)

        def h(o):
            return lax.rem(t - o + 4 * NH, NH)

        H, F, z, zm = s.H, s.F, s.z, s.zm
        k, kr = lax.rem(t, NS), lax.rem(t + NS - D, NS)
        RY, RR, RL = s.RY.at[kr], s.RR.at[kr], s.RL.at[kr]
        SY, SR, SL = s.SY.at[k], s.SR.at[k], s.SL.at[k]

        own = (h(D), slice(None), pl.ds(s.a0, A))
        H[own] = H[own] + RY[:, 0 : 6 * L].astype(f32)
        rooted = H[h(4 * D), :, pl.ds(s.b_own, L)] + RY[:, 6 * L : 7 * L].astype(f32)
        F[f(4 * D), :, pl.ds(s.b_own, L)] = rooted.astype(bf)
        F[f(5 * D), :, pl.ds(s.b_oth, L)] = RY[:, 7 * L : 8 * L]
        F[f(5 * D + D * z), :, pl.ds(s.o0, A2)] = RY[:, 8 * L : 11 * L]
        F[f(5 * D + D * zm), :, pl.ds(s.o3, A2)] = RY[:, 11 * L : 14 * L]
        to_r = jnp.where(s.has_l, RR[:, 11 * L :].astype(f32), 0.0) + H[h(D + D * z), :, pl.ds(s.a3, A2)]
        to_l = jnp.where(s.has_r, RL[:, : 3 * L].astype(f32), 0.0) + H[h(D + D * zm), :, pl.ds(s.a0, A2)]
        to_r, to_l = to_r.astype(bf), to_l.astype(bf)
        f3 = jnp.where(s.has_r, RL[:, 11 * L :], to_r)
        f0 = jnp.where(s.has_l, RR[:, : 3 * L], to_l)
        F[f(4 * D + D * zm), :, pl.ds(s.a3, A2)] = f3
        F[f(4 * D + D * z), :, pl.ds(s.a0, A2)] = f0
        SR[:, 11 * L :], SR[:, : 3 * L] = to_r, f0
        SL[:, : 3 * L], SL[:, 11 * L :] = to_l, f3
        SY[:, 8 * L : 11 * L], SY[:, 11 * L :] = f0, f3
        hr, hl = h(D * z), h(D * zm)
        here, at = pl.ds(s.bz, BT), pl.ds(pl.multiple_of(s.bz - BO + A2, L), BT)
        H[hr, :, here] = H[hr, :, here] + jnp.where(s.has_l, RR[:, at].astype(f32), 0.0)
        H[hl, :, here] = H[hl, :, here] + jnp.where(s.has_r, RL[:, at].astype(f32), 0.0)
        for q in range(4):
            b = pl.ds(BO + q * BT, BT)
            m = pl.ds(A2 + q * BT, BT)
            fq = f(5 * D + D * jnp.abs(z - q))
            done = F[fq, :, b]
            if q < 3:
                done = jnp.where(z > q, RR[:, m], done)
            if q > 0:
                done = jnp.where(z < q, RL[:, m], done)
            F[fq, :, b] = done
            if q > 0:
                sum_r = H[hr, :, b] + jnp.where(s.has_l, RR[:, m].astype(f32), 0.0)
                SR[:, m] = jnp.where(z < q, sum_r.astype(bf), done)
            else:
                SR[:, m] = done
            if q < 3:
                sum_l = H[hl, :, b] + jnp.where(s.has_r, RL[:, m].astype(f32), 0.0)
                SL[:, m] = jnp.where(z > q, sum_l.astype(bf), done)
            else:
                SL[:, m] = done
        s.messages(t, always, lambda c: c.start(), (0, s.has_r), (1, s.has_l))
        SY[:, : 6 * L] = H[h(0), :, pl.ds(s.o0, A)].astype(bf)
        SY[:, 6 * L : 7 * L] = H[h(3 * D), :, pl.ds(s.b_oth, L)].astype(bf)
        SY[:, 7 * L : 8 * L] = F[f(4 * D), :, pl.ds(s.b_own, L)]
        s.messages(t, always, lambda c: c.start(), (2, always))

        @pl.when(t >= 8 * D)
        def _():
            for c in s.outs(t - 8 * D):
                c.start()

        pl.when(t >= 8 * D + W)(lambda: s.wait_outs(t - 8 * D - W))

        @pl.when(t + AHEAD < NB)
        def _():
            b = t + AHEAD
            own, partner = s.loads(b)
            pl.when(lax.rem(b, BPG) == 0)(lambda: s.wait_partner(b // BPG))
            pl.when(b >= DIRECT)(lambda: own.start())
            partner.start()

        pl.when(t + 1 < NB)(lambda: s.chip_sum(t + 1))

    def finish(s):
        for b in range(NB - W, NB):
            s.wait_outs(b)
        for t in range(STEPS - D - NS + D, STEPS - D):
            s.message(2, t, False).wait_send()
            pl.when(s.has_r)(lambda t=t: s.message(0, t, False).wait_send())
            pl.when(s.has_l)(lambda t=t: s.message(1, t, False).wait_send())


    def weights(s):
        def copy(src, dst, sem):
            return pltpu.make_async_copy(src, dst, sem)

        first, quarters = [], []
        for j in range(4):
            at = (slice(None), pl.ds(j * Q, Q))
            first.append(copy(s.wd_h.at[at], s.WD.at[at], s.wd.at[j]))
        for j in range(4):
            rows = pl.ds(s.quarter(j), Q)
            quarters.append(
                [
                    copy(w.at[rows], s.WGU.at[rows, pl.ds(n * FF, FF)], s.wgu.at[j, n])
                    for n, w in enumerate((s.wg, s.wu))
                ]
            )
        return first, quarters

    def quarter(s, j):
        mine = jnp.where(j < 2, 1 - s.side, s.side)
        return pl.multiple_of(mine * HC + lax.rem(j, 2) * Q, Q)

    def dy_part(s, g, j):
        return pl.ds(pl.multiple_of(lax.rem(g, 2) * 4 * G + j * G, G), G)

    def group_loads(s, g):
        k = lax.rem(g, 2)
        rows = pl.ds(pl.multiple_of(g * G, G), G)
        parts = [
            pltpu.make_async_copy(
                s.dy.at[rows, pl.ds(j * Q, Q)], s.POOL.at[s.dy_part(g, j), pl.ds(0, Q)], s.ld.at[k, j]
            )
            for j in range(4)
        ]
        return parts + [
            pltpu.make_async_copy(a.at[rows], v.at[k], s.ld.at[k, 4 + n])
            for n, (a, v) in enumerate(((s.gate, s.GA), (s.up, s.UP)))
        ]

    def to_partner(s, g, j):
        rows = pl.ds(pl.multiple_of(g * G, G), G)
        return pltpu.make_async_remote_copy(
            src_ref=s.PST.at[j],
            dst_ref=s.pt.at[rows, pl.ds(pl.multiple_of(j * Q, Q), Q)],
            send_sem=s.ps.at[j],
            recv_sem=s.pr.at[g, j],
            device_id={"tp": s.cid},
            device_id_type=MESH,
        )

    def to_own(s, g, j):
        rows = pl.ds(pl.multiple_of(g * G, G), G)
        dst = s.own.at[rows, pl.ds(pl.multiple_of(j * Q, Q), Q)]
        return pltpu.make_async_copy(s.OST.at[j], dst, s.ow.at[j])

    def wait_partner(s, g):
        for j in range(2):
            s.to_partner(g, j).wait_recv()

    def hidden(s, g, lo, hi, arrive=None):
        k = lax.rem(g, 2)
        rows = pl.ds(pl.multiple_of(g * G, G), G)
        d = 0.0
        for j in range(4):
            if arrive:
                arrive(j)
            d += dot(s.POOL[s.dy_part(g, j), 0:Q], s.WD[lo:hi, j * Q : (j + 1) * Q], 1, 1)
        a, u = s.GA[k, :, lo:hi].astype(f32), s.UP[k, :, lo:hi].astype(f32)
        sig = jax.nn.sigmoid(a)
        silu = a * sig
        s.DGU[rows, lo:hi] = (d * u * (sig + silu * (1.0 - sig))).astype(bf)
        s.DGU[rows, FF + lo : FF + hi] = (d * silu).astype(bf)
        s.HID[rows, lo:hi] = (silu * u).astype(bf)

    def term(s, g, j):
        rows = pl.ds(pl.multiple_of(g * G, G), G)
        return dot(s.DGU[rows, :], s.WGU[pl.ds(s.quarter(j), Q), :], 1, 1)

    def direct(s, lo, hi):
        for b in range(lo, hi):
            for j in range(2):
                s.H[b, :, j * Q : (j + 1) * Q] = s.OST[j, b * R : (b + 1) * R, :]

    def before1(s, u):
        g, r = u // PPG, lax.rem(u, PPG)

        @pl.when(((r == 0) & (u >= 2 * PPG)) | (u == PPG + 2))
        def _():
            for j in range(2):
                s.to_partner(g - 1, j).wait_send()
                s.to_own(g - 1, j).wait()

        @pl.when(u == LEAD - 1)
        def _():
            s.wait_partner(0)
            for b in range(AHEAD):
                s.loads(b)[1].start()

        @pl.when(u == LEAD)
        def _():
            s.direct(0, 2)
            s.chip_sum(jnp.int32(0))

        @pl.when((u == LEAD) & (s.side == 1))
        def _():
            pl.delay(700)

        @pl.when((r == 0) & (g + 1 < NG))
        def _():
            for c in s.group_loads(g + 1):
                c.start(priority=1)

    def piece1(s, u):
        g, r = u // PPG, lax.rem(u, PPG)
        first, quarters = s.weights()

        @pl.when(r == 0)
        def _():
            copies = s.group_loads(g)

            def arrive(n):
                copies[n].wait()

                @pl.when(g == 0)
                def _():
                    first[n].wait()
                    for c in quarters[n]:
                        c.start(priority=1)

                if n == 3:
                    copies[4].wait()
                    copies[5].wait()

            s.hidden(g, 0, F0, arrive)

        pl.when(r == 1)(lambda: s.hidden(g, F0, FF))
        for j in range(4):

            @pl.when(u == 2 + j)
            def _(j=j):
                for c in quarters[j]:
                    c.wait()

        @pl.when((r == 2) | (r == 3))
        def _():
            j = r - 2
            s.PST[j] = s.term(g, j).astype(bf)
            s.to_partner(g, j).start()

        @pl.when(r >= 4)
        def _():
            j = r - 4
            s.OST[j] = s.term(g, r - 2)
            s.to_own(g, j).start()


    def x_tile(s, q):
        k = lax.rem(q, 2)
        v = s.POOL.at[:, pl.ds(pl.multiple_of(k * XT, XT), XT)]
        src = s.x.at[:, pl.ds(pl.multiple_of(q * XT, XT), XT)]
        return v, pltpu.make_async_copy(src, v, s.xl.at[k])

    def y_tile(s, q):
        k = lax.rem(q, 2)
        v = s.POOL.at[:, pl.ds(pl.multiple_of(2 * XT + k * YT, XT), YT)]
        src = s.dy.at[:, pl.ds(pl.multiple_of(q * YT, YT), YT)]
        return v, pltpu.make_async_copy(src, v, s.yl.at[k])

    def half_tile(s, q):
        k, n = lax.rem(q, 2), YT // 2
        v = s.POOL.at[:, pl.ds(pl.multiple_of(2 * XT + k * YT, XT), n)]
        src = s.dy.at[:, pl.ds(pl.multiple_of(WIDE * YT + q * n, n), n)]
        return v, pltpu.make_async_copy(src, v, s.yl.at[k])

    def piece2(s, u):
        m = u - P2

        @pl.when(m < NX)
        def _():
            pl.when(m + 1 < NX)(lambda: s.x_tile(m + 1)[1].start(priority=1))
            tile, load = s.x_tile(m)
            load.wait()
            rows = pl.ds(pl.multiple_of(m * XT, XT), XT)
            s.WGU[rows, :] = dot(tile[...], s.DGU[...], 0, 0).astype(bf)

        @pl.when((m >= NX) & (m < NX + WIDE))
        def _():
            q = m - NX
            pl.when(q + 1 < WIDE)(lambda: s.y_tile(q + 1)[1].start(priority=1))
            pl.when(q + 1 == WIDE)(lambda: s.half_tile(0)[1].start(priority=1))
            tile, load = s.y_tile(q)
            load.wait()
            columns = pl.ds(pl.multiple_of(q * YT, YT), YT)
            s.WD[:, columns] = dot(s.HID[...], tile[...], 0, 0).astype(bf)

        @pl.when(m >= NX + WIDE)
        def _():
            q = m - NX - WIDE
            pl.when(m + 1 < PIECES2)(lambda: s.half_tile(q + 1)[1].start(priority=1))
            tile, load = s.half_tile(q)
            load.wait()
            n = YT // 2
            columns = pl.ds(pl.multiple_of(WIDE * YT + q * n, n), n)
            s.WD[:, columns] = dot(s.HID[...], tile[...], 0, 0).astype(bf)

    def run(s):
        first, _ = s.weights()
        group = s.group_loads(0)
        for n in range(4):
            group[n].start()
            first[n].start()
        group[4].start()
        group[5].start()
        s.barrier()

        def iteration(u, _):
            pl.when(u <= P2)(lambda: s.before1(u))
            pl.when(u >= LEAD)(lambda: s.service(u - LEAD))
            pl.when(u == LEAD)(lambda: s.direct(2, DIRECT))

            @pl.when(u == P2 - 3)
            def _():
                s.x_tile(0)[1].start(priority=1)
                s.y_tile(0)[1].start(priority=1)

            pl.when(u < P2)(lambda: s.piece1(u))
            pl.when((u >= P2) & (u < P2 + PIECES2))(lambda: s.piece2(u))
            return 0

        lax.fori_loop(0, LEAD + STEPS, iteration, 0)
        s.finish()


XC, WC, YC = 16, 8, 8
SLOTS, LAG = 7, 2


def copy_out(dx, dwgu, dwd, dx_out, dwg_out, dwu_out, dwd_out, mid, rd, wr, gs, us, ys):
    def part(n, k, j):
        return pl.ds(j * (n // k), n // k)

    def read(j):
        at = part(T_ROWS, XC, j)
        return pltpu.make_async_copy(dx.at[at], mid.at[j % SLOTS], rd.at[j])

    def write(j):
        at = part(T_ROWS, XC, j)
        return pltpu.make_async_copy(mid.at[j % SLOTS], dx_out.at[at], wr.at[j])

    rest = []
    for j in range(WC):
        at = part(D_MODEL, WC, j)
        rest.append(pltpu.make_async_copy(dwgu.at[at, pl.ds(0, FF)], dwg_out.at[at], gs.at[j]))
        rest.append(pltpu.make_async_copy(dwgu.at[at, pl.ds(FF, FF)], dwu_out.at[at], us.at[j]))
        at = part(FF, YC, j)
        rest.append(pltpu.make_async_copy(dwd.at[at], dwd_out.at[at], ys.at[j]))
    for j in range(SLOTS):
        read(j).start()
    n = 0
    for j in range(XC):
        read(j).wait()
        write(j).start()
        for c in rest[n : (j + 1) * len(rest) // XC]:
            c.start()
        n = (j + 1) * len(rest) // XC
        if j >= LAG and j - LAG + SLOTS < XC:
            write(j - LAG).wait()
            read(j - LAG + SLOTS).start()
    for c in rest:
        c.wait()
    for j in range(XC - SLOTS, XC):
        write(j).wait()


def solution(mesh):
    def step(x, dy, gate, up, w_gate, w_up, w_down):
        shape = jax.ShapeDtypeStruct
        anywhere = pl.BlockSpec(memory_space=pl.ANY)
        vmem = pl.BlockSpec(memory_space=pltpu.VMEM)
        dx, dw_gu, dw_down, _, _ = pl.pallas_call(
            lambda *refs: Kernel(*refs).run(),
            out_shape=[
                shape((T_ROWS, D_MODEL), bf),
                pltpu.VMEM((D_MODEL, 2 * FF), bf),
                pltpu.VMEM((FF, D_MODEL), bf),
                shape((T_ROWS, HC), f32),
                shape((T_ROWS, HC), bf),
            ],
            in_specs=[anywhere] * 7,
            out_specs=[anywhere, vmem, vmem, anywhere, anywhere],
            scratch_shapes=list(SCRATCH.values()),
            compiler_params=pltpu.CompilerParams(
                collective_id=0, has_side_effects=True, vmem_limit_bytes=37 << 20
            ),
            name="mlp_backward",
        )(x, dy, gate, up, w_gate, w_up, w_down)
        return pl.pallas_call(
            copy_out,
            out_shape=[
                shape((T_ROWS, D_MODEL), bf),
                shape((D_MODEL, FF), bf),
                shape((D_MODEL, FF), bf),
                shape((FF, D_MODEL), bf),
            ],
            in_specs=[anywhere, vmem, vmem],
            out_specs=[anywhere] * 4,
            scratch_shapes=[
                pltpu.VMEM((SLOTS, T_ROWS // XC, D_MODEL), bf),
                DMA((XC,)),
                DMA((XC,)),
                DMA((WC,)),
                DMA((WC,)),
                DMA((YC,)),
            ],
            compiler_params=pltpu.CompilerParams(vmem_limit_bytes=10 << 20),
            name="copy_out",
        )(dx, dw_gu, dw_down)

    tokens, columns, rows = P("dp", None), P(None, "tp"), P("tp", None)
    return jax.shard_map(
        step,
        mesh=mesh,
        in_specs=(tokens, tokens, P("dp", "tp"), P("dp", "tp"), columns, columns, rows),
        out_specs=(tokens, P("dp", "tp"), P("dp", "tp"), P(("dp", "tp"), None)),
        check_vma=False,
    )
```
